32 devices in a mesh: grp: 2 (over y), tile: 4 (over z), coil: 2 (over x), spk: 2 (over core).
Axes of the slice: x: 2, y: 2, z: 4, core: 2. Of those that a mesh axis runs over, the one named last changes fastest.
Arguments:
- coil_maps: float32 [2, 512, 2, 256], P('coil', ('grp', 'tile', 'spk')), parts along dimension 1, may hold values from -6 to 6
- kspace_data: bfloat16 [2, 128, 2, 256], P('coil', ('grp', 'tile', 'spk')), parts along dimension 1, may hold values from -24 to 24
- interp_weights: bfloat16 [128, 6, 256], P(('grp', 'tile', 'spk')), parts along dimension 0, may hold values from 0.099609375 to 1
- sample_bins: int32 [128, 256], P(('grp', 'tile', 'spk')), parts along dimension 0, may hold values from 0 to 65535, as said below
- spoke_count: int32 [16], P(('grp', 'tile', 'spk')), parts along dimension 0, may hold values from 1 to 8, 32 in all
- thresholds: float32 [3], replicated, may hold values from 0.05 to 0.3
Outputs:
- image: float32 [512, 2, 256], P(('grp', 'tile', 'spk')), parts along dimension 0
The draws below stay inside these ranges and needn't reach their ends.
There are 2 independent parts, one for each index of `grp`. The reference program is written for one: setup_inputs(seed, part) draws one part's arguments, and reference() takes and returns one part's arrays. A program takes and returns all parts, laid end to end along the dimension named above; an argument that names none is the same for every part. Nothing has to cross between parts.
Inputs may be any that keep to these rules, and one draw needn't show every extreme that they name: `sample_bins`: sample k of each spoke lies on a straight line through cell (128, 128), at offset k - 128 along the spoke's direction, coordinates taken modulo 256. `spoke_count`: each independent slice has its own 8 counts, and the whole array holds one such block of counts per slice. The 8 counts of each slice sum to 32. In every draw, at least one device of each slice holds 8 live spokes. A device's live spokes are its first ones.
All inputs are finite; a program needn't handle non-finite values.
Results may differ from the reference program's by a relative error of at most 0.0016.
Values may be sent and summed in bfloat16 or wider, within the bound.
A program may use at most 64 MiB of HBM per device.

```python
import math
import jax
import jax.numpy as jnp
import numpy as np
from jax import lax

N = 256
RO = 256
SPK_DEV = 8
LEVELS = 3
ITERS = 4
COILS = 2
BLOCKS = 8
SPOKES = 64


def draw_sample_bins(key, part):
    key_side, key_sign, key_slope = jax.random.split(key, 3)
    middle = N // 2
    side_pick = jax.random.randint(key_side, (SPOKES,), 0, 2)
    sign_pick = jax.random.randint(key_sign, (SPOKES,), 0, 2) * 2 - 1
    slope_val = jax.random.randint(key_slope, (SPOKES,), -middle, middle + 1)
    row_dir = jnp.where(side_pick == 1, sign_pick * middle, slope_val)
    col_dir = jnp.where(side_pick == 1, slope_val, sign_pick * middle)
    offsets = jnp.arange(RO, dtype=jnp.int32) - RO // 2
    row_bins = (middle + offsets[None, :] * row_dir[:, None] * 2 // RO) % N
    col_bins = (middle + offsets[None, :] * col_dir[:, None] * 2 // RO) % N
    return (row_bins * N + col_bins).astype(jnp.int32)


def steps_of(stream_key, dims, cuts, least, high):
    factor_of, own = 1.0, jax.random.fold_in(stream_key, 6)
    for position, parts in cuts:
        steps = jnp.exp(jax.random.uniform(jax.random.fold_in(own, position), (parts,), jnp.float32, least / len(cuts), high / len(cuts)))
        factor_of = factor_of * jnp.repeat(steps, dims[position] // parts).reshape([-1 if axis == position else 1 for axis in range(len(dims))])
    return factor_of


def profile(number_of, total, most, lean):
    portions = [(1 << 20) // math.isqrt(grade ** lean) + 1 for grade in range(2, number_of + 1)]
    surplus, holding = total - most - (number_of - 1), [1] * (number_of - 1)
    while surplus > 0:
        movable = [i for i in range(number_of - 1) if holding[i] < most]
        whole, left = sum([portions[i] for i in movable]), surplus
        for i in movable:
            addition = min(most - holding[i], max(1, left * portions[i] // whole), surplus)
            holding[i] = holding[i] + addition
            surplus = surplus - addition
    return np.array([most] + holding)


def uneven(rng, number_of, total, reach, skew):
    if number_of == 2:
        one = jax.random.randint(rng, (), max(1, total - reach), min(reach, total - 1) + 1)
        return jnp.stack([one, total - one])
    sizes = jnp.asarray(profile(number_of, total, reach, skew), jnp.int32)
    twos = (number_of - 1) // 2
    giver, sink = sizes[1:1 + 2 * twos:2], sizes[2:2 + 2 * twos:2]
    margin = jnp.minimum(giver - 1, reach - sink)
    passed = jax.random.randint(jax.random.fold_in(rng, 1), (twos,), 0, 1 << 20) % (margin + 1)
    sizes = sizes.at[1:1 + 2 * twos:2].set(giver - passed).at[2:2 + 2 * twos:2].set(sink + passed)
    return sizes[jax.random.permutation(jax.random.fold_in(rng, 2), number_of)]


def gaussian(rng, dims, spread, limit, pieces=(), kind=jnp.bfloat16):
    entries = jax.random.normal(rng, dims, jnp.float32) * spread
    if len(pieces) > 0:
        entries = steps_of(rng, dims, pieces, -0.22, 0.18) * entries
    return jnp.clip(entries, min=-limit, max=limit).astype(kind)


def setup_inputs(seed: int = 0, part: int = 0) -> dict:
    splits = jax.random.split(jax.random.key(seed), 7)
    own_keys = jax.random.split(jax.random.fold_in(splits[6], part), 7)
    return {
        "coil_maps": gaussian(own_keys[0], (COILS, N, 2, N), (1.0 / (2.0 * COILS) ** 0.5), 6.0, ((0, 2), (1, 8)), jnp.float32),
        "kspace_data": gaussian(own_keys[1], (COILS, SPOKES, 2, RO), 4.0, 24.0, ((0, 2), (1, 8))),
        "interp_weights": jnp.clip(0.099609375 + 0.9003906 * jax.random.uniform(own_keys[2], (SPOKES, 6, RO), jnp.float32) ** steps_of(own_keys[2], (SPOKES, 6, RO), ((0, 8),), -0.2, 0.2), 0.099609375, 1.0).astype(jnp.bfloat16),
        "sample_bins": draw_sample_bins(jax.random.fold_in(jax.random.fold_in(splits[6], part), 71), part),
        "spoke_count": uneven(own_keys[4], BLOCKS, BLOCKS * SPK_DEV // 2, SPK_DEV, 2).astype(jnp.int32),
        "thresholds": jnp.clip(jax.random.uniform(splits[5], (LEVELS,), jnp.float32, 0.05, 0.3), 0.05, 0.3),
    }


HIGH = lax.Precision.HIGHEST
STEP_SIZE = 0.5
RSQRT2 = 0.7071067811865476

def dft_table(length, direction):
    positions = jnp.arange(length, dtype=jnp.int32)
    phases = positions[:, None] * positions[None, :] % length
    angles = phases.astype(jnp.float32) * jnp.float32(2.0 * math.pi / length)
    norm_scale = 1.0 / math.sqrt(length)
    cosine = jnp.cos(angles) * norm_scale
    sine_tab = jnp.sin(angles) * norm_scale
    top_rows = jnp.stack([cosine, -direction * sine_tab], axis=1)
    bottom = jnp.stack([direction * sine_tab, cosine], axis=1)
    return jnp.stack([top_rows, bottom], axis=0)

def haar_matrix(length, levels):
    haar_mat = jnp.eye(length, dtype=jnp.float32)
    positions = jnp.arange(length, dtype=jnp.int32)
    out_i = positions[:, None]
    in_j = positions[None, :]
    for level_num in range(levels):
        span_len = length >> level_num
        half_len = span_len // 2
        low_hit = (out_i < half_len) & ((in_j == 2 * out_i) | (in_j == 2 * out_i + 1))
        high_pos = out_i - half_len
        high_hit = (out_i >= half_len) & (out_i < span_len) & ((in_j == 2 * high_pos) | (in_j == 2 * high_pos + 1))
        sign_val = jnp.where(in_j == 2 * high_pos + 1, -1.0, 1.0)
        step_mat = jnp.where(low_hit, RSQRT2, jnp.where(high_hit, sign_val * RSQRT2, 0.0))
        step_mat = step_mat + jnp.where((out_i >= span_len) & (in_j == out_i), 1.0, 0.0)
        haar_mat = jnp.dot(step_mat.astype(jnp.float32), haar_mat, precision=HIGH)
    return haar_mat

def haar_labels(length, levels):
    positions = jnp.arange(length, dtype=jnp.int32)
    band_label = jnp.ones((length,), jnp.int32)
    for level_num in range(1, levels + 1):
        band_label = band_label + (positions < length >> level_num).astype(jnp.int32)
    return band_label

def wavelet_shrink(target, thresholds, levels):
    row_count, pair_dim, col_count = target.shape
    block_len = 2 ** levels
    row_haar = haar_matrix(block_len, levels)
    col_haar = haar_matrix(col_count, levels)
    grouped = target.reshape(row_count // block_len, block_len, pair_dim, col_count)
    coeffs = jnp.einsum('ij,gjpc->gipc', row_haar, grouped, precision=HIGH)
    coeffs = jnp.einsum('gipc,kc->gipk', coeffs, col_haar, precision=HIGH)
    band_min = jnp.minimum(haar_labels(block_len, levels)[:, None], haar_labels(col_count, levels)[None, :])
    active = band_min <= levels
    limits = jnp.ones(band_min.shape, jnp.float32)
    for level_num in range(levels):
        limits = jnp.where(band_min == level_num + 1, thresholds[level_num], limits)
    magnitude = jnp.sqrt(coeffs[:, :, 0] ** 2 + coeffs[:, :, 1] ** 2)
    factor = jnp.maximum(magnitude - limits, 0.0) / jnp.maximum(magnitude, limits)
    factor = jnp.where(active, factor, 1.0)
    shrunk = coeffs * factor[:, :, None, :]
    restored = jnp.einsum('gipk,kc->gipc', shrunk, col_haar, precision=HIGH)
    restored = jnp.einsum('ij,gipc->gjpc', row_haar, restored, precision=HIGH)
    return restored.reshape(row_count, pair_dim, col_count)

def complex_mul(left, right):
    real_part = left[:, 0] * right[:, 0] - left[:, 1] * right[:, 1]
    imag_part = left[:, 0] * right[:, 1] + left[:, 1] * right[:, 0]
    return jnp.stack([real_part, imag_part], axis=1)

def conj_mul(left, right):
    real_part = left[:, 0] * right[:, 0] + left[:, 1] * right[:, 1]
    imag_part = left[:, 0] * right[:, 1] - left[:, 1] * right[:, 0]
    return jnp.stack([real_part, imag_part], axis=1)

def reference(coil_maps, kspace_data, interp_weights, sample_bins, spoke_count, thresholds):
    spokes_all = sample_bins.shape[0]
    blocks_all = spoke_count.shape[0]
    per_block = spokes_all // blocks_all
    live_total = spokes_all // 2
    spoke_ids = jnp.arange(spokes_all, dtype=jnp.int32)
    owners = (spoke_ids // per_block).astype(jnp.int32)
    live_mask = (spoke_ids % per_block < spoke_count[owners]).astype(jnp.float32)
    offset = jnp.abs(jnp.arange(RO, dtype=jnp.int32) - RO // 2).astype(jnp.float32)
    density = (offset + 0.5) * (N / (3.0 * RO * live_total))
    row_bins = sample_bins // N
    col_bins = sample_bins % N
    row_taps = [((row_bins + tap_index - 1) % N).astype(jnp.int32) for tap_index in range(3)]
    col_taps = [((col_bins + tap_index - 1) % N).astype(jnp.int32) for tap_index in range(3)]
    weights_f = interp_weights.astype(jnp.float32)
    fwd_table = dft_table(N, 1.0)
    inv_table = dft_table(N, -1.0)

    def coil_gradient(estimate, maps_one, data_one):
        coil_image = complex_mul(maps_one, estimate)
        half_done = jnp.einsum('rpc,pcqv->rqv', coil_image, fwd_table, precision=HIGH)
        kspace = jnp.einsum('rpv,prqu->vqu', half_done, fwd_table, precision=HIGH).astype(jnp.bfloat16)
        kspace = lax.optimization_barrier(kspace).astype(jnp.float32)
        sample_model = jnp.zeros((spokes_all, RO, 2), jnp.float32)
        for col_index in range(3):
            inner_sum = jnp.zeros((spokes_all, RO, 2), jnp.float32)
            for row_index in range(3):
                picked = kspace[col_taps[col_index], :, row_taps[row_index]]
                inner_sum = inner_sum + weights_f[:, row_index, :, None] * picked
            sample_model = sample_model + weights_f[:, 3 + col_index, :, None] * inner_sum
        sample_model = jnp.transpose(sample_model, (0, 2, 1))
        weighted = live_mask[:, None, None] * density[None, None, :] * (sample_model - data_one.astype(jnp.float32))
        gridded = jnp.zeros((N, 2, N), jnp.float32)
        for col_index in range(3):
            smeared = (weights_f[:, 3 + col_index, None, :] * weighted).astype(jnp.bfloat16)
            smeared = lax.optimization_barrier(smeared).astype(jnp.float32)
            smeared_t = jnp.transpose(smeared, (0, 2, 1))
            for row_index in range(3):
                gridded = gridded.at[col_taps[col_index], :, row_taps[row_index]].add(weights_f[:, row_index, :, None] * smeared_t)
        partial_back = jnp.einsum('vpu,puqr->vqr', gridded, inv_table, precision=HIGH)
        coil_back = jnp.einsum('vpr,pvqc->rqc', partial_back, inv_table, precision=HIGH)
        return conj_mul(maps_one, coil_back)
    estimate = jnp.zeros((N, 2, N), jnp.float32)
    for iteration in range(ITERS):
        terms = lax.map(lambda coil_pack: coil_gradient(estimate, coil_pack[0], coil_pack[1]), (coil_maps, kspace_data))
        gradient = lax.optimization_barrier(jnp.sum(terms, axis=0))
        estimate = wavelet_shrink(estimate - STEP_SIZE * gradient, thresholds, LEVELS)
    return estimate
```

```python
import functools
import math

import jax
import jax.numpy as jnp
import numpy as np
from jax import lax
from jax.experimental import pallas as pl
from jax.experimental.pallas import tpu as pltpu
from jax.sharding import PartitionSpec as P

SPK_DEV = 8
LEVELS = 3
MEMBERS = 2**LEVELS
ITERS = 4
CORES = 2
GROUP = 2
TAPS = 3
FIELDS = 8
MARGIN = 16
STEP_SIZE = 0.5
LANES = 128
TINY = 1e-30
F32 = jnp.float32
BF16 = jnp.bfloat16
MESH = pl.DeviceIdType.MESH

_scope = [None]


def mark(name):
    if _scope[0] is not None:
        _scope[0].__exit__(None, None, None)
        _scope[0] = None
    if name:
        _scope[0] = jax.named_scope(name)
        _scope[0].__enter__()


def split_np(table):
    table = np.ascontiguousarray(table).astype(np.float32)
    high = table.astype(jnp.bfloat16)
    low = (table - high.astype(np.float32)).astype(jnp.bfloat16)
    return high, low


def haar_signs(length, levels):
    mat = np.eye(length)
    for level in range(levels):
        span = length >> level
        half = span // 2
        step = np.eye(length)
        step[:span] = 0.0
        for i in range(half):
            step[i, 2 * i] = step[i, 2 * i + 1] = 1.0
            step[half + i, 2 * i] = 1.0
            step[half + i, 2 * i + 1] = -1.0
        mat = step @ mat
    return mat


def haar_labels(length, levels):
    label = np.ones((length,), np.int32)
    for level in range(1, levels + 1):
        label = label + (np.arange(length) < length >> level)
    return label


def mirror(first, n):
    second = (n - first) % n
    second[first == 0] = n // 2
    return np.concatenate([first, second])


def orders(n):
    half = n // 2
    by_lane = mirror(np.arange(half), n)
    edge = MARGIN // 2
    near = np.concatenate([np.arange(edge), np.arange(half - edge, half), np.arange(edge, half - edge)])
    by_freq = mirror(near, n)
    groups = half // MEMBERS
    member = np.arange(half) // groups
    group = np.arange(half) % groups
    low = MEMBERS * group + member
    high = n - MEMBERS * group - member
    high[:groups] = n - MEMBERS * (np.arange(groups) + 1)
    by_pixel = np.concatenate([low, high])
    return by_lane, by_freq, low, by_pixel


def tables(n):
    half = n // 2
    by_lane, by_freq, low, by_pixel = orders(n)
    phase = np.outer(np.arange(n), np.arange(n)) % n
    angle = phase * (2.0 * np.pi / n)
    cosine = np.cos(angle) / math.sqrt(n)
    sine = np.sin(angle) / math.sqrt(n)

    def folded(outs, ins):
        bottom = sine[outs][:, ins]
        bottom[outs == 0] = cosine[half][ins]
        return np.concatenate([cosine[outs][:, ins], bottom], axis=0)

    right = folded(np.arange(half), by_lane).T
    back = folded(low, by_freq)
    fore = folded(by_freq[:half], by_pixel)
    small = haar_signs(MEMBERS, LEVELS)
    chunk_haar = []
    for q in range(2):
        pixels = by_lane[q * half : (q + 1) * half]
        mat = np.zeros((half, half))
        group = pixels // MEMBERS - q * (half // MEMBERS)
        for k in range(MEMBERS):
            mat[group * MEMBERS + k, np.arange(half)] = small[k, pixels % MEMBERS]
        both = np.kron(np.eye(2), mat)
        chunk_haar.append((both.T, both))
    haar = np.stack([np.stack(pair) for pair in chunk_haar]).astype(jnp.bfloat16)
    windows = np.stack(
        [by_freq[: half + MARGIN], np.concatenate([by_freq[half:], by_freq[:MARGIN]])]
    )
    cell_u = np.repeat(by_lane[:, None], LANES, axis=1).astype(jnp.bfloat16)
    cell_v = np.repeat(windows[:, :, None], LANES, axis=2).astype(jnp.bfloat16)
    turn_s = np.zeros((n, n))
    turn_s[np.arange(n), by_pixel] = 1.0
    turn_r = np.zeros((n, n))
    turn_r[np.arange(n), by_lane] = 1.0
    perms = np.stack([turn_s, turn_r]).astype(jnp.bfloat16)
    return (
        np.stack(split_np(right)), np.stack(split_np(back)), np.stack(split_np(fore)),
        haar, cell_u, cell_v, perms,
    )


def split(x):
    high = x.astype(BF16)
    return high, (x - high.astype(F32)).astype(BF16)


def mm(a, b):
    return jnp.dot(a, b, preferred_element_type=F32)


def mm_t(a, b):
    return lax.dot_general(a, b, (((1,), (1,)), ((), ())), preferred_element_type=F32)


def mm3(a, b):
    return mm(a[0], b[0]) + (mm(a[0], b[1]) + mm(a[1], b[0]))


def forward_haar(x):
    sums = [x[2 * i] + x[2 * i + 1] for i in range(4)]
    out = [None] * 4 + [x[2 * i] - x[2 * i + 1] for i in range(4)]
    pair = [sums[0] + sums[1], sums[2] + sums[3]]
    out[2], out[3] = sums[0] - sums[1], sums[2] - sums[3]
    out[0], out[1] = pair[0] + pair[1], pair[0] - pair[1]
    return out


def inverse_haar(c):
    pair = [c[0] + c[1], c[0] - c[1]]
    sums = [pair[0] + c[2], pair[0] - c[2], pair[1] + c[3], pair[1] - c[3]]
    out = []
    for i in range(4):
        out += [sums[i] + c[4 + i], sums[i] - c[4 + i]]
    return out


def kernel(
    dims,
    thr_ref, count_ref, weight_ref, bins_ref, data_ref, map_ref,
    right_hbm, back_hbm, fore_hbm, haar_hbm, cell_u_hbm, cell_v_hbm, perm_hbm,
    out_ref,
    right, back, fore, haar, cell_u, cell_v, perms,
    meta_mine, meta_all, data_mine, data_all, map_mine, maps,
    wide_meta, pairs, pair_data, row_tab, col_tab, kspace, grid, smeared,
    half_h, half_l, estimate, grads, sens,
    const_sem, meta_send, meta_recv, data_send, data_recv, map_send, map_recv, grad_send, grad_recv,
):
    n, tiles, coils, rows, live = dims
    half = n // 2
    window = half + MARGIN
    blocks = tiles * CORES
    slots = blocks * SPK_DEV
    pair_count = live // 2
    coil, tile, core = lax.axis_index("coil"), lax.axis_index("tile"), lax.axis_index("spk")
    pair, bit = coil // CORES, coil % CORES
    block = tile * CORES + core
    mine = pair * CORES + core

    mark("start")
    const_copies = []
    for k, (src, dst) in enumerate((
        (cell_u_hbm, cell_u), (cell_v_hbm, cell_v), (right_hbm, right), (back_hbm, back),
        (perm_hbm, perms), (haar_hbm, haar), (fore_hbm, fore),
    )):
        copy = pltpu.make_async_copy(src, dst, const_sem.at[k])
        copy.start()
        const_copies.append(copy)

    barrier = pltpu.get_barrier_semaphore()
    peers = [
        (d_bit, d_tile, d_core)
        for d_bit in range(CORES)
        for d_tile in range(tiles)
        for d_core in range(CORES)
        if d_bit + d_tile + d_core > 0
    ]
    for d_bit, d_tile, d_core in peers:
        pl.semaphore_signal(
            barrier,
            inc=1,
            device_id={
                "coil": pair * CORES + (bit + d_bit) % CORES,
                "tile": (tile + d_tile) % tiles,
                "spk": (core + d_core) % CORES,
            },
            device_id_type=MESH,
        )
    for d in range(CORES, coils):
        pl.semaphore_signal(
            barrier,
            inc=1,
            device_id={
                "coil": (coil + d // CORES * CORES) % coils,
                "spk": (core + d % CORES) % CORES,
            },
            device_id_type=MESH,
        )

    mark("prep")
    alive = lax.broadcasted_iota(jnp.int32, (SPK_DEV, n), 0) < count_ref[0]
    bins = bins_ref[...]
    row_of = jnp.where(alive, bins // n, -1).astype(F32)
    col_of = (bins % n).astype(F32)
    for j in range(0, SPK_DEV, 2):
        parts = []
        for i in (j, j + 1):
            parts += [weight_ref[i].astype(F32), row_of[i : i + 1], col_of[i : i + 1]]
        meta_mine[j * FIELDS : (j + 2) * FIELDS] = jnp.concatenate(parts, axis=0).astype(BF16)
    data_wide = data_ref[0].astype(F32)
    data_mine[...] = jnp.concatenate([data_wide[:, 0], data_wide[:, 1]], axis=0).astype(BF16)
    for p in range(2):
        map_mine[p] = map_ref[0, :, p, :]

    mark("barrier")
    pl.semaphore_wait(barrier, len(peers) + coils - CORES)

    mark("issue")
    sends = []
    for d_tile in range(tiles):
        for d_core in range(CORES):
            if d_tile == 0 and d_core == 0:
                continue
            copy = pltpu.make_async_remote_copy(
                src_ref=meta_mine,
                dst_ref=meta_all.at[block],
                send_sem=meta_send.at[d_tile * CORES + d_core],
                recv_sem=meta_recv.at[block],
                device_id={"tile": (tile + d_tile) % tiles, "spk": (core + d_core) % CORES},
                device_id_type=MESH,
            )
            copy.start()
            sends.append(copy)
    across_core = []
    for src, dst, s_sem, r_sem in (
        (data_mine, data_all.at[block], data_send, data_recv),
        (map_mine, maps.at[:, block], map_send, map_recv),
    ):
        for d_bit in range(CORES):
            for d_tile in range(tiles):
                copy = pltpu.make_async_remote_copy(
                    src_ref=src,
                    dst_ref=dst,
                    send_sem=s_sem.at[d_bit * tiles + d_tile],
                    recv_sem=r_sem.at[block],
                    device_id={
                        "coil": pair * CORES + (bit + d_bit) % CORES,
                        "tile": (tile + d_tile) % tiles,
                        "spk": bit,
                    },
                    device_id_type=MESH,
                )
                if d_bit == 0 and d_tile == 0:
                    local_copy = pltpu.make_async_copy(src, dst, r_sem.at[block])

                    @pl.when(core == bit)
                    def _(local_copy=local_copy):
                        local_copy.start()

                    @pl.when(core != bit)
                    def _(copy=copy):
                        copy.start()

                    across_core.append(copy)
                else:
                    copy.start()
                    sends.append(copy)

    mark("metawait")
    for copy in const_copies:
        copy.wait()
    meta_all[block] = meta_mine[...]
    for d_block in range(1, blocks):
        other = (block + d_block) % blocks
        pltpu.make_async_copy(meta_all.at[other], meta_all.at[other], meta_recv.at[other]).wait()

    mark("rank")
    flat = meta_all[...].reshape(slots * FIELDS, n).astype(F32)
    for t in range(n // LANES):
        wide_meta[t] = flat[:, t * LANES : (t + 1) * LANES]

    def field(m):
        return jnp.concatenate(
            [wide_meta[t, pl.ds(m, slots, stride=FIELDS), :] for t in range(n // LANES)], axis=1
        )

    rows_all = field(2 * TAPS)
    up = lax.broadcasted_iota(jnp.int32, (slots, slots), 0)
    across = lax.broadcasted_iota(jnp.int32, (slots, slots), 1)
    flag = jnp.where(rows_all[:, :LANES] >= 0.0, 1.0 / LANES, 0.0)
    flags = mm_t(jnp.ones((live, LANES), BF16), flag.astype(BF16)).astype(BF16)
    rank = mm(flags, jnp.where(up < across, 1.0, 0.0).astype(BF16))
    here = lax.broadcasted_iota(jnp.int32, (live, slots), 0).astype(F32)
    hit = (flags.astype(F32) > 0.5) & (rank == here)
    pick = jnp.where(hit, 1.0, 0.0).astype(BF16)
    comp = [mm(pick, (rows_all if m == 2 * TAPS else field(m)).astype(BF16)) for m in range(FIELDS)]
    first_low = jnp.broadcast_to(comp[2 * TAPS + 1][:, 1:2], (live, half)) < half

    def halves(x):
        low = jnp.where(first_low, x[:, :half], x[:, half:])
        high = jnp.where(first_low, x[:, half:], x[:, :half])
        return [jnp.concatenate([v[:pair_count], v[pair_count:]], axis=1) for v in (low, high)]

    for m in range(2 * TAPS):
        for o, value in enumerate(halves(comp[m])):
            pairs[o, m] = value
    for m, centre in ((2 * TAPS, comp[2 * TAPS]), (3 * TAPS, comp[2 * TAPS + 1])):
        for t in range(TAPS):
            tap = (centre.astype(jnp.int32) + (t - 1)) & (n - 1)
            for o, value in enumerate(halves(tap.astype(F32))):
                pairs[o, m + t] = value

    mark("build")

    def build(i, carry):
        def table(cells, m, o):
            def part(k):
                return jnp.broadcast_to(pairs[o, k, pl.ds(i, 1), :].astype(BF16), cells.shape)

            zero = jnp.zeros(cells.shape, BF16)
            return jnp.where(
                cells == part(2 * TAPS + m), part(m),
                jnp.where(
                    cells == part(2 * TAPS + m + 1), part(m + 1),
                    jnp.where(cells == part(2 * TAPS + m + 2), part(m + 2), zero),
                ),
            )

        for o in range(2):
            cells = jnp.concatenate([cell_u[...]] * (n // LANES), axis=1)
            row_tab[i, o] = table(cells, 0, o)
            cells = jnp.concatenate([cell_v[o]] * (n // LANES), axis=1)
            col_tab[i, o] = table(cells, TAPS, o)
        return carry

    lax.fori_loop(0, pair_count, build, 0)

    mark("datawait")
    for b in range(blocks):
        pltpu.make_async_copy(data_all.at[b], data_all.at[b], data_recv.at[b]).wait()
    offset = jnp.abs(lax.broadcasted_iota(jnp.int32, (live, n), 1) - half).astype(F32)
    density = (offset + 0.5) * (n / (3.0 * n * live))
    for o, value in enumerate(halves(density)):
        pair_data[o, 2] = value
    every = data_all[...]
    for p in range(2):
        samples = jnp.concatenate(
            [every[b].astype(F32)[p * SPK_DEV : (p + 1) * SPK_DEV] for b in range(blocks)], axis=0
        )
        for o, value in enumerate(halves(mm(pick, samples.astype(BF16)))):
            pair_data[o, p] = value

    first_lane = lax.broadcasted_iota(jnp.int32, (n, half), 1) == 0
    first_row = lax.broadcasted_iota(jnp.int32, (half, half), 0) == 0
    groups = half // MEMBERS
    label = haar_labels(MEMBERS, LEVELS)
    lane = lax.broadcasted_iota(jnp.int32, (1, half), 1) % MEMBERS
    lane_label = jnp.ones((1, half), jnp.int32)
    for level in range(1, LEVELS + 1):
        lane_label = lane_label + jnp.where(lane < MEMBERS >> level, 1, 0)

    def norm_of(k):
        return 1.0 / math.sqrt((haar_signs(MEMBERS, LEVELS)[k] ** 2).sum())

    lane_norm = jnp.zeros((1, half), F32)
    for k in range(MEMBERS):
        lane_norm = jnp.where(lane == k, norm_of(k), lane_norm)
    limits, scales = [], []
    for k in range(MEMBERS):
        band = jnp.minimum(lane_label, int(label[k]))
        limit = jnp.zeros((1, half), F32)
        for level in range(LEVELS):
            limit = jnp.where(band == level + 1, thr_ref[level], limit)
        limits.append(limit)
        scales.append(lane_norm * norm_of(k))

    for it in range(ITERS):
        slot = it % 2
        mark("spokes")
        grid[...] = jnp.zeros_like(grid)

        def fore_step(step, into, it=it):
            for g in range(GROUP):
                i = step * GROUP + g
                for o in range(2):
                    col = col_tab[i, o].astype(F32)
                    dens = pair_data[o, 2, pl.ds(i, 1), :]
                    inner = mm(kspace[o], row_tab[i, o]) if it > 0 else None
                    for p in range(2):
                        value = -pair_data[o, p, pl.ds(i, 1), :]
                        if it > 0:
                            value = value + jnp.sum(
                                inner[p * window : (p + 1) * window] * col, axis=0, keepdims=True
                            )
                        smeared[into, o, p * window : (p + 1) * window, g * n : (g + 1) * n] = (
                            col * (dens * value)
                        ).astype(BF16)

        def back_step(step, source):
            for o in range(2):
                total = None
                for g in range(GROUP):
                    added = mm_t(
                        smeared[source, o, :, g * n : (g + 1) * n], row_tab[step * GROUP + g, o]
                    )
                    total = added if total is None else total + added
                grid[o] += total

        steps = pair_count // GROUP
        fore_step(0, 0)

        def body(step, carry):
            into = step % 2
            fore_step(step, into)
            back_step(step - 1, 1 - into)
            return carry

        lax.fori_loop(1, steps, body, 0)
        back_step(steps - 1, (steps - 1) % 2)

        mark("turned")
        stack = []
        for p in range(2):
            low, high = grid[0, p * window : (p + 1) * window], grid[1, p * window : (p + 1) * window]
            stack += [
                low[:MARGIN] + high[half:], low[MARGIN:half],
                high[:MARGIN] + low[half:], high[MARGIN:half],
            ]
        turned = mm3(split(jnp.concatenate(stack, axis=0)), (right[0], right[1]))
        r_c, i_c = turned[:n, :half], turned[n:, :half]
        r_s, i_s = turned[:n, half:], turned[n:, half:]
        r_z, i_z = jnp.where(first_lane, 0.0, r_s), jnp.where(first_lane, 0.0, i_s)
        sides = [
            split(jnp.concatenate([r_c - i_z, i_c + r_z], axis=1)),
            split(jnp.concatenate(
                [jnp.where(first_lane, r_s, r_c + i_s), jnp.where(first_lane, i_s, i_c - r_s)], axis=1
            )),
        ]
        if it == 0:
            mark("mapwait")
            for b in range(blocks):
                pltpu.make_async_copy(maps.at[:, b], maps.at[:, b], map_recv.at[b]).wait()
            for p in range(2):
                plain = split(maps[p].reshape(n, n))
                moved = split(sum(mm(perms[1], x) for x in plain))
                both = sum(mm_t(perms[0], x) for x in moved)
                for q in range(2):
                    sens[p, q] = both[:, q * half : (q + 1) * half]

        mark("image")
        copies = []
        for q in range(2):
            w = mm3((back[0], back[1]), sides[q])
            c_r, c_i, s_r, s_i = w[:half, :half], w[:half, half:], w[half:, :half], w[half:, half:]
            z_r, z_i = jnp.where(first_row, 0.0, s_r), jnp.where(first_row, 0.0, s_i)
            low_r, low_i = c_r - z_i, c_i + z_r
            high_r = jnp.where(first_row, s_r, c_r + s_i)
            high_i = jnp.where(first_row, s_i, c_i - s_r)
            d_r = jnp.concatenate(
                [low_r, pltpu.roll(high_r[:groups], groups - 1, 0), high_r[groups:]], axis=0
            )
            d_i = jnp.concatenate(
                [low_i, pltpu.roll(high_i[:groups], groups - 1, 0), high_i[groups:]], axis=0
            )
            m_r, m_i = sens[0, q], sens[1, q]
            grads[slot, q, mine, 0] = m_r * d_r + m_i * d_i
            grads[slot, q, mine, 1] = m_r * d_i - m_i * d_r
            for d in range(1, coils):
                d_pair, d_core = d // CORES, d % CORES
                copy = pltpu.make_async_remote_copy(
                    src_ref=grads.at[slot, q, mine],
                    dst_ref=grads.at[slot, q, mine],
                    send_sem=grad_send.at[slot, q, d],
                    recv_sem=grad_recv.at[slot, q, mine],
                    device_id={
                        "coil": (coil + d_pair * CORES) % coils,
                        "spk": (core + d_core) % CORES,
                    },
                    device_id_type=MESH,
                )
                copy.start()
                copies.append(copy)

        for q in range(2):
            mark("gradwait")
            for d in range(1, coils):
                d_pair, d_core = d // CORES, d % CORES
                other = (coil + d_pair * CORES) % coils // CORES * CORES + (core + d_core) % CORES
                pltpu.make_async_copy(
                    grads.at[slot, q, other], grads.at[slot, q, other], grad_recv.at[slot, q, other]
                ).wait()
            mark("shrink")
            summed = grads[slot, q, 0]
            for c in range(1, coils):
                summed = summed + grads[slot, q, c]
            target = -STEP_SIZE * jnp.concatenate([summed[0], summed[1]], axis=1)
            if it > 0:
                target = estimate[q] + target

            def piece(x, h, m):
                first = h * half + (m if h == 0 else (MEMBERS - m) % MEMBERS) * groups
                return x[first : first + groups]

            along = []
            for h in range(2):
                along += forward_haar([piece(target, h, m) for m in range(MEMBERS)])
            side = split(jnp.concatenate(along, axis=0))
            coeffs = mm(side[0], haar[q, 0]) + mm(side[1], haar[q, 0])
            shrunk = []
            for h in range(2):
                for k in range(MEMBERS):
                    first = h * half + k * groups
                    c_r = coeffs[first : first + groups, :half] * scales[k]
                    c_i = coeffs[first : first + groups, half:] * scales[k]
                    power = jnp.maximum(c_r * c_r + c_i * c_i, TINY)
                    factor = jnp.maximum(1.0 - limits[k] * lax.rsqrt(power), 0.0) * scales[k]
                    shrunk.append(jnp.concatenate([c_r * factor, c_i * factor], axis=1))
            side = split(jnp.concatenate(shrunk, axis=0))
            along = mm(side[0], haar[q, 1]) + mm(side[1], haar[q, 1])
            fresh = []
            for h in range(2):
                first = h * half
                members = inverse_haar(
                    [along[first + k * groups : first + (k + 1) * groups] for k in range(MEMBERS)]
                )
                placed = [None] * MEMBERS
                for m in range(MEMBERS):
                    placed[m if h == 0 else (MEMBERS - m) % MEMBERS] = members[m]
                fresh += placed
            fresh = jnp.concatenate(fresh, axis=0)
            estimate[q] = fresh
            if it < ITERS - 1:
                mark("fwd")
                e_r, e_i = fresh[:, :half], fresh[:, half:]
                m_r, m_i = sens[0, q], sens[1, q]
                seen = split(
                    jnp.concatenate([m_r * e_r - m_i * e_i, m_r * e_i + m_i * e_r], axis=1)
                )
                w = mm3((fore[0], fore[1]), seen)
                c_r, c_i, s_r, s_i = w[:half, :half], w[:half, half:], w[half:, :half], w[half:, half:]
                z_r, z_i = jnp.where(first_row, 0.0, s_r), jnp.where(first_row, 0.0, s_i)
                v = jnp.concatenate(
                    [
                        c_r + z_i, jnp.where(first_row, s_r, c_r - s_i),
                        c_i - z_r, jnp.where(first_row, s_i, c_i + s_r),
                    ],
                    axis=0,
                )
                half_h[:, q * half : (q + 1) * half], half_l[:, q * half : (q + 1) * half] = split(v)
        mark("sendwait")
        for copy in copies:
            copy.wait_send()
        if it < ITERS - 1:
            mark("vfft")
            v = mm3((half_h[...], half_l[...]), (right[0], right[1]))
            r_c, i_c, r_s, i_s = v[:n, :half], v[n:, :half], v[:n, half:], v[n:, half:]
            r_z, i_z = jnp.where(first_lane, 0.0, r_s), jnp.where(first_lane, 0.0, i_s)
            whole = [
                jnp.concatenate([r_c + i_z, jnp.where(first_lane, r_s, r_c - i_s)], axis=1).astype(BF16),
                jnp.concatenate([i_c - r_z, jnp.where(first_lane, i_s, i_c + r_s)], axis=1).astype(BF16),
            ]
            for p in range(2):
                first = p * window
                kspace[0, first : first + window] = whole[p][:window]
                kspace[1, first : first + half] = whole[p][half:]
                kspace[1, first + half : first + window] = whole[p][:MARGIN]

    mark("out")
    take = lax.broadcasted_iota(jnp.int32, (rows, n), 0) + block * rows
    at = lax.broadcasted_iota(jnp.int32, (rows, n), 1)
    owner = jnp.where(at <= half, at, n + half - at)
    chosen = jnp.where(take == owner, 1.0, 0.0).astype(BF16)
    for p in range(2):
        mine_rows = jnp.concatenate([estimate[q, :, p * half : (p + 1) * half] for q in range(2)], axis=1)
        picked = sum(mm_t(chosen, x) for x in split(mine_rows))
        out_ref[:, p, :] = sum(mm(x, perms[0]) for x in split(picked))

    @pl.when(core != bit)
    def _():
        for copy in across_core:
            copy.wait_send()

    for copy in sends:
        copy.wait_send()
    mark(None)


def local(coil_maps, kspace_data, interp_weights, sample_bins, spoke_count, thresholds):
    tiles, coils = lax.axis_size("tile"), lax.axis_size("coil")
    blocks = tiles * CORES
    rows, n = coil_maps.shape[1], coil_maps.shape[3]
    live = blocks * SPK_DEV // 2
    half = n // 2
    window = half + MARGIN
    consts = tables(n)
    vmem = pl.BlockSpec(memory_space=pltpu.VMEM)
    smem = pl.BlockSpec(memory_space=pltpu.SMEM)
    slots = blocks * SPK_DEV
    pair_count = live // 2
    dma = pltpu.SemaphoreType.DMA
    return pl.pallas_call(
        functools.partial(kernel, (n, tiles, coils, rows, live)),
        out_shape=jax.ShapeDtypeStruct((rows, 2, n), F32),
        in_specs=[smem, smem] + [vmem] * 4 + [pl.BlockSpec(memory_space=pl.ANY)] * len(consts),
        out_specs=vmem,
        scratch_shapes=[pltpu.VMEM(c.shape, BF16) for c in consts] + [
            pltpu.VMEM((SPK_DEV * FIELDS, n), BF16),
            pltpu.VMEM((blocks, SPK_DEV * FIELDS, n), BF16),
            pltpu.VMEM((SPK_DEV * 2, n), BF16),
            pltpu.VMEM((blocks, SPK_DEV * 2, n), BF16),
            pltpu.VMEM((2, rows, n), F32),
            pltpu.VMEM((2, blocks, rows, n), F32),
            pltpu.VMEM((n // LANES, slots * FIELDS, LANES), F32),
            pltpu.VMEM((2, 4 * TAPS, pair_count, n), F32),
            pltpu.VMEM((2, 3, pair_count, n), F32),
            pltpu.VMEM((pair_count, 2, n, n), BF16),
            pltpu.VMEM((pair_count, 2, window, n), BF16),
            pltpu.VMEM((2, 2 * window, n), BF16),
            pltpu.VMEM((2, 2 * window, n), F32),
            pltpu.VMEM((2, 2, 2 * window, GROUP * n), BF16),
            pltpu.VMEM((2 * n, n), BF16),
            pltpu.VMEM((2 * n, n), BF16),
            pltpu.VMEM((2, n, n), F32),
            pltpu.VMEM((2, 2, coils, 2, n, half), F32),
            pltpu.VMEM((2, 2, n, half), F32),
            dma((len(consts),)),
            dma((blocks,)), dma((blocks,)), dma((blocks,)), dma((blocks,)),
            dma((blocks,)), dma((blocks,)),
            dma((2, 2, coils)), dma((2, 2, coils)),
        ],
        compiler_params=pltpu.CompilerParams(
            has_side_effects=True, collective_id=0, vmem_limit_bytes=60 * 1024 * 1024
        ),
    )(thresholds, spoke_count, interp_weights, sample_bins, kspace_data, coil_maps, *consts)


def solution(mesh):
    placed = (
        P("coil", ("grp", "tile", "spk"), None, None),
        P("coil", ("grp", "tile", "spk"), None, None),
        P(("grp", "tile", "spk"), None, None),
        P(("grp", "tile", "spk"), None),
        P(("grp", "tile", "spk")),
        P(),
    )
    return jax.shard_map(
        local,
        mesh=mesh,
        in_specs=placed,
        out_specs=P(("grp", "tile", "spk"), None, None),
        check_vma=False,
    )
```

```python
import functools
import math

import jax
import jax.numpy as jnp
import numpy as np
from jax import lax
from jax.experimental import pallas as pl
from jax.experimental.pallas import tpu as pltpu
from jax.sharding import PartitionSpec as P

SPK_DEV = 8
LEVELS = 3
MEMBERS = 2**LEVELS
ITERS = 4
CORES = 2
GROUP = 2
TAPS = 3
FIELDS = 8
MARGIN = 16
STEP_SIZE = 0.5
LANES = 128
TINY = 1e-30
VMEM_LIMIT = 60 * 1024 * 1024
F32 = jnp.float32
BF16 = jnp.bfloat16
MESH = pl.DeviceIdType.MESH

_scope = [None]


def mark(name):
    if _scope[0] is not None:
        _scope[0].__exit__(None, None, None)
        _scope[0] = None
    if name:
        _scope[0] = jax.named_scope(name)
        _scope[0].__enter__()


def split_np(table):
    table = np.ascontiguousarray(table).astype(np.float32)
    high = table.astype(jnp.bfloat16)
    low = (table - high.astype(np.float32)).astype(jnp.bfloat16)
    return high, low


def haar_signs(length, levels):
    mat = np.eye(length)
    for level in range(levels):
        span = length >> level
        half = span // 2
        step = np.eye(length)
        step[:span] = 0.0
        for i in range(half):
            step[i, 2 * i] = step[i, 2 * i + 1] = 1.0
            step[half + i, 2 * i] = 1.0
            step[half + i, 2 * i + 1] = -1.0
        mat = step @ mat
    return mat


def haar_labels(length, levels):
    label = np.ones((length,), np.int32)
    for level in range(1, levels + 1):
        label = label + (np.arange(length) < length >> level)
    return label


def mirror(first, n):
    second = (n - first) % n
    second[first == 0] = n // 2
    return np.concatenate([first, second])


def orders(n):
    half = n // 2
    by_lane = mirror(np.arange(half), n)
    edge = MARGIN // 2
    near = np.concatenate([np.arange(edge), np.arange(half - edge, half), np.arange(edge, half - edge)])
    by_freq = mirror(near, n)
    groups = half // MEMBERS
    member = np.arange(half) // groups
    group = np.arange(half) % groups
    low = MEMBERS * group + member
    high = n - MEMBERS * group - member
    high[:groups] = n - MEMBERS * (np.arange(groups) + 1)
    by_pixel = np.concatenate([low, high])
    return by_lane, by_freq, low, by_pixel


def tables(n):
    half = n // 2
    by_lane, by_freq, low, by_pixel = orders(n)
    phase = np.outer(np.arange(n), np.arange(n)) % n
    angle = phase * (2.0 * np.pi / n)
    cosine = np.cos(angle) / math.sqrt(n)
    sine = np.sin(angle) / math.sqrt(n)

    def folded(outs, ins):
        bottom = sine[outs][:, ins]
        bottom[outs == 0] = cosine[half][ins]
        return np.concatenate([cosine[outs][:, ins], bottom], axis=0)

    right = folded(np.arange(half), by_lane).T
    back = folded(low, by_freq)
    fore = folded(by_freq[:half], by_pixel)
    small = haar_signs(MEMBERS, LEVELS)
    chunk_haar = []
    for q in range(2):
        pixels = by_lane[q * half : (q + 1) * half]
        mat = np.zeros((half, half))
        group = pixels // MEMBERS - q * (half // MEMBERS)
        for k in range(MEMBERS):
            mat[group * MEMBERS + k, np.arange(half)] = small[k, pixels % MEMBERS]
        both = np.kron(np.eye(2), mat)
        chunk_haar.append((both.T, both))
    haar = np.stack([np.stack(pair) for pair in chunk_haar]).astype(jnp.bfloat16)
    windows = np.stack(
        [by_freq[: half + MARGIN], np.concatenate([by_freq[half:], by_freq[:MARGIN]])]
    )
    cell_u = np.repeat(by_lane[:, None], LANES, axis=1).astype(jnp.bfloat16)
    cell_v = np.repeat(windows[:, :, None], LANES, axis=2).astype(jnp.bfloat16)
    turn_s = np.zeros((n, n))
    turn_s[np.arange(n), by_pixel] = 1.0
    turn_r = np.zeros((n, n))
    turn_r[np.arange(n), by_lane] = 1.0
    perms = np.stack([turn_s, turn_r]).astype(jnp.bfloat16)
    return (
        np.stack(split_np(right)), np.stack(split_np(back)), np.stack(split_np(fore)),
        haar, cell_u, cell_v, perms,
    )


def split(x):
    high = x.astype(BF16)
    return high, (x - high.astype(F32)).astype(BF16)


def mm(a, b):
    return jnp.dot(a, b, preferred_element_type=F32)


def mm_t(a, b):
    return lax.dot_general(a, b, (((1,), (1,)), ((), ())), preferred_element_type=F32)


def mm3(a, b):
    return mm(a[0], b[0]) + (mm(a[0], b[1]) + mm(a[1], b[0]))


def forward_haar(x):
    sums = [x[2 * i] + x[2 * i + 1] for i in range(4)]
    out = [None] * 4 + [x[2 * i] - x[2 * i + 1] for i in range(4)]
    pair = [sums[0] + sums[1], sums[2] + sums[3]]
    out[2], out[3] = sums[0] - sums[1], sums[2] - sums[3]
    out[0], out[1] = pair[0] + pair[1], pair[0] - pair[1]
    return out


def inverse_haar(c):
    pair = [c[0] + c[1], c[0] - c[1]]
    sums = [pair[0] + c[2], pair[0] - c[2], pair[1] + c[3], pair[1] - c[3]]
    out = []
    for i in range(4):
        out += [sums[i] + c[4 + i], sums[i] - c[4 + i]]
    return out


def kernel(
    dims,
    thr_ref, count_ref, weight_hbm, bins_hbm, data_hbm, map_hbm,
    right_hbm, back_hbm, fore_hbm, haar_hbm, cell_u_hbm, cell_v_hbm, perm_hbm,
    out_ref,
    right, back, fore, haar, cell_u, cell_v, perms,
    bins_ref, data_ref, map_ref, meta_mine, meta_all, data_mine, data_all, map_mine, maps,
    pairs, pair_data, row_tab, col_tab, kspace, grid, smear_a, smear_b,
    half_h, half_l, estimate, grads, sens,
    const_sem, arg_sem, meta_send, meta_recv, data_send, data_recv, map_send, map_recv, grad_send, grad_recv,
):
    n, tiles, coils, rows, live = dims
    half = n // 2
    window = half + MARGIN
    blocks = tiles * CORES
    slots = blocks * SPK_DEV
    pair_count = live // 2
    coil, tile, core = lax.axis_index("coil"), lax.axis_index("tile"), lax.axis_index("spk")
    pair, bit = coil // CORES, coil % CORES
    block = tile * CORES + core
    mine = pair * CORES + core

    def toggled(value, d):
        step = 1
        while step <= d:
            if d & step:
                value = value + step - 2 * step * (value // step % 2)
            step *= 2
        return value

    mark("start")
    barrier = pltpu.get_barrier_semaphore()
    peers = [
        (d_bit, d_tile, d_core)
        for d_bit in range(CORES)
        for d_tile in range(tiles)
        for d_core in range(CORES)
        if (d_tile > 0 and d_bit == 0) or (d_tile < 2 and d_tile + d_bit + d_core > 0)
    ]
    for d_bit, d_tile, d_core in peers:
        pl.semaphore_signal(
            barrier,
            inc=1,
            device_id={
                "coil": pair * CORES + (bit + d_bit) % CORES,
                "tile": toggled(tile, d_tile),
                "spk": (core + d_core) % CORES,
            },
            device_id_type=MESH,
        )
    for d in range(CORES, coils):
        pl.semaphore_signal(
            barrier,
            inc=1,
            device_id={
                "coil": (coil + d // CORES * CORES) % coils,
                "spk": (core + d % CORES) % CORES,
            },
            device_id_type=MESH,
        )
    arg_copies = []
    for k, (src, dst) in enumerate((
        (bins_hbm, bins_ref), (weight_hbm, meta_mine.at[: 2 * TAPS]),
        (data_hbm, data_ref), (map_hbm, map_ref),
    )):
        copy = pltpu.make_async_copy(src, dst, arg_sem.at[k])
        copy.start()
        arg_copies.append(copy)
    const_copies = []
    for k, (src, dst) in enumerate((
        (perm_hbm, perms), (cell_u_hbm, cell_u), (cell_v_hbm, cell_v), (right_hbm, right),
        (back_hbm, back), (haar_hbm, haar), (fore_hbm, fore),
    )):
        copy = pltpu.make_async_copy(src, dst, const_sem.at[k])
        copy.start()
        const_copies.append(copy)

    mark("prep")
    for copy in arg_copies:
        copy.wait()
    alive = lax.broadcasted_iota(jnp.int32, (SPK_DEV, n), 0) < count_ref[0]
    bins = bins_ref[...]
    row_of = jnp.where(alive, bins // n, -1).astype(F32)
    col_of = (bins % n).astype(F32)
    meta_mine[2 * TAPS] = row_of.astype(BF16)
    meta_mine[2 * TAPS + 1] = col_of.astype(BF16)
    data_wide = data_ref[0].astype(F32)
    data_mine[...] = jnp.concatenate([data_wide[:, 0], data_wide[:, 1]], axis=0).astype(BF16)
    mark("barrier")
    pl.semaphore_wait(barrier, len(peers) + coils - CORES)

    mark("issue")
    sends = []
    near = [toggled(tile, d) for d in range(tiles)]
    far_first = list(range(tiles // 2, tiles)) + list(range(1, tiles // 2))

    def send(src, dst, s_sem, r_sem, target):
        copy = pltpu.make_async_remote_copy(
            src_ref=src, dst_ref=dst, send_sem=s_sem, recv_sem=r_sem,
            device_id=target, device_id_type=MESH,
        )
        copy.start()
        return copy

    for d in far_first:
        sends.append(send(
            meta_mine, meta_all.at[block], meta_send.at[d], meta_recv.at[block], {"tile": near[d]}
        ))
    sends.append(send(
        meta_mine, meta_all.at[block], meta_send.at[0], meta_recv.at[block], {"spk": 1 - core}
    ))
    inner = []
    across = pair * CORES + 1 - bit
    routes = [{"coil": across, "spk": bit}, {"tile": near[1], "spk": bit},
              {"coil": across, "tile": near[1], "spk": bit}]
    routes += [{"tile": near[d], "spk": bit} for d in far_first if d > 1]

    def spread(src, dst, s_sem, r_sem):
        for k, route in enumerate(routes):
            sends.append(send(src, dst, s_sem.at[1 + k], r_sem, route))
        local_copy = pltpu.make_async_copy(src, dst, r_sem)
        inner_copy = pltpu.make_async_remote_copy(
            src_ref=src, dst_ref=dst, send_sem=s_sem.at[0], recv_sem=r_sem,
            device_id={"spk": 1 - core}, device_id_type=MESH,
        )
        inner.append(inner_copy)

        @pl.when(core == bit)
        def _():
            local_copy.start()

        @pl.when(core != bit)
        def _():
            inner_copy.start()

    spread(data_mine, data_all.at[block], data_send, data_recv.at[block])
    const_copies[0].wait()
    for p in range(2):
        map_mine[p] = sum(mm_t(x, perms[0]) for x in split(map_ref[0, :, p, :]))
    spread(map_mine, maps.at[:, block], map_send, map_recv.at[block])

    def arrived(ref, sem):
        pltpu.make_async_copy(ref, ref, sem).wait()

    def hand_over(ref, s_sem, r_sem):
        return (
            pltpu.make_async_copy(ref, ref, r_sem),
            pltpu.make_async_remote_copy(
                src_ref=ref, dst_ref=ref, send_sem=s_sem, recv_sem=r_sem,
                device_id={"coil": across}, device_id_type=MESH,
            ),
        )

    map_hand, data_hand = [], []
    for d in far_first:
        if d < 2:
            continue
        for c in range(CORES):
            b = near[d] * CORES + c
            k = 2 + tiles + len(map_hand)
            map_hand.append(hand_over(maps.at[:, b], map_send.at[k], map_recv.at[b]))
            data_hand.append(hand_over(data_all.at[b], data_send.at[k], data_recv.at[b]))

    def pass_on(hands):
        @pl.when(core == bit)
        def _():
            for here, there in hands:
                here.wait()
                there.start()

    mark("metawait")
    for copy in const_copies[1:]:
        copy.wait()
    meta_all[block] = meta_mine[...]
    for d in range(1, tiles):
        b = near[d] * CORES + core
        arrived(meta_all.at[b], meta_recv.at[b])
        sends.append(send(
            meta_all.at[b], meta_all.at[b], meta_send.at[tiles + d], meta_recv.at[b], {"spk": 1 - core}
        ))
    for d in range(tiles):
        b = near[d] * CORES + 1 - core
        arrived(meta_all.at[b], meta_recv.at[b])

    mark("pass")

    pass_on(data_hand)
    direct = [near[d] * CORES + c for d in range(2) for c in range(CORES)]

    @pl.when(core == bit)
    def _():
        for b in direct:
            arrived(data_all.at[b], data_recv.at[b])

    mark("rank")
    whole = [meta_all[b].reshape(FIELDS * SPK_DEV, n).astype(F32) for b in range(blocks)]

    def field(m):
        return jnp.concatenate([w[m * SPK_DEV : (m + 1) * SPK_DEV] for w in whole], axis=0)

    rows_all = field(2 * TAPS)
    up = lax.broadcasted_iota(jnp.int32, (slots, slots), 0)
    across = lax.broadcasted_iota(jnp.int32, (slots, slots), 1)
    flag = jnp.where(rows_all[:, :LANES] >= 0.0, 1.0 / LANES, 0.0)
    flags = mm_t(jnp.ones((live, LANES), BF16), flag.astype(BF16)).astype(BF16)
    rank = mm(flags, jnp.where(up < across, 1.0, 0.0).astype(BF16))
    here = lax.broadcasted_iota(jnp.int32, (live, slots), 0).astype(F32)
    hit = (flags.astype(F32) > 0.5) & (rank == here)
    pick = jnp.where(hit, 1.0, 0.0).astype(BF16)
    comp = [mm(pick, (rows_all if m == 2 * TAPS else field(m)).astype(BF16)) for m in range(FIELDS)]
    first_low = jnp.broadcast_to(comp[2 * TAPS + 1][:, 1:2], (live, half)) < half

    def halves(x):
        low = jnp.where(first_low, x[:, :half], x[:, half:])
        high = jnp.where(first_low, x[:, half:], x[:, :half])
        return [jnp.concatenate([v[:pair_count], v[pair_count:]], axis=1) for v in (low, high)]

    for m in range(2 * TAPS):
        for o, value in enumerate(halves(comp[m])):
            pairs[o, m] = value
    for m, centre in ((2 * TAPS, comp[2 * TAPS]), (3 * TAPS, comp[2 * TAPS + 1])):
        for t in range(TAPS):
            tap = (centre.astype(jnp.int32) + (t - 1)) & (n - 1)
            for o, value in enumerate(halves(tap.astype(F32))):
                pairs[o, m + t] = value

    stage = len(map_hand) // 2
    pass_on(map_hand[:stage])
    mark("build")

    def build(i, carry):
        def table(cells, m, o):
            def part(k):
                return jnp.broadcast_to(pairs[o, k, pl.ds(i, 1), :].astype(BF16), cells.shape)

            zero = jnp.zeros(cells.shape, BF16)
            return jnp.where(
                cells == part(2 * TAPS + m), part(m),
                jnp.where(
                    cells == part(2 * TAPS + m + 1), part(m + 1),
                    jnp.where(cells == part(2 * TAPS + m + 2), part(m + 2), zero),
                ),
            )

        for o in range(2):
            cells = jnp.concatenate([cell_u[...]] * (n // LANES), axis=1)
            row_tab[i, o] = table(cells, 0, o)
            cells = jnp.concatenate([cell_v[o]] * (n // LANES), axis=1)
            col_tab[i, o] = table(cells, TAPS, o)
        return carry

    lax.fori_loop(0, pair_count, build, 0)

    mark("datawait")
    pass_on(map_hand[stage:])

    @pl.when(core != bit)
    def _():
        for b in range(blocks):
            arrived(data_all.at[b], data_recv.at[b])

    offset = jnp.abs(lax.broadcasted_iota(jnp.int32, (live, n), 1) - half).astype(F32)
    density = (offset + 0.5) * (n / (3.0 * n * live))
    for o, value in enumerate(halves(density)):
        pair_data[o, 2] = value
    every = data_all[...]
    for p in range(2):
        samples = jnp.concatenate(
            [every[b].astype(F32)[p * SPK_DEV : (p + 1) * SPK_DEV] for b in range(blocks)], axis=0
        )
        for o, value in enumerate(halves(mm(pick, samples.astype(BF16)))):
            pair_data[o, p] = value

    first_lane = lax.broadcasted_iota(jnp.int32, (n, half), 1) == 0
    first_row = lax.broadcasted_iota(jnp.int32, (half, half), 0) == 0
    groups = half // MEMBERS
    label = haar_labels(MEMBERS, LEVELS)
    lane = lax.broadcasted_iota(jnp.int32, (1, half), 1) % MEMBERS
    lane_label = jnp.ones((1, half), jnp.int32)
    for level in range(1, LEVELS + 1):
        lane_label = lane_label + jnp.where(lane < MEMBERS >> level, 1, 0)

    def norm_of(k):
        return 1.0 / math.sqrt((haar_signs(MEMBERS, LEVELS)[k] ** 2).sum())

    lane_norm = jnp.zeros((1, half), F32)
    for k in range(MEMBERS):
        lane_norm = jnp.where(lane == k, norm_of(k), lane_norm)
    limits, scales = [], []
    for k in range(MEMBERS):
        band = jnp.minimum(lane_label, int(label[k]))
        limit = jnp.zeros((1, half), F32)
        for level in range(LEVELS):
            limit = jnp.where(band == level + 1, thr_ref[level], limit)
        limits.append(limit)
        scales.append(lane_norm * norm_of(k))

    copies = []
    for it in range(ITERS):
        slot = it % 2
        mark("spokes")
        grid[...] = jnp.zeros_like(grid)

        def fore_step(step, into, it=it):
            for g in range(GROUP):
                i = step * GROUP + g
                for o in range(2):
                    col = col_tab[i, o].astype(F32)
                    dens = pair_data[o, 2, pl.ds(i, 1), :]
                    seen = mm(kspace[o], row_tab[i, o]) if it > 0 else None
                    for p in range(2):
                        value = -pair_data[o, p, pl.ds(i, 1), :]
                        if it > 0:
                            value = value + jnp.sum(
                                seen[p * window : (p + 1) * window] * col, axis=0, keepdims=True
                            )
                        into[o, p * window : (p + 1) * window, g * n : (g + 1) * n] = (
                            col * (dens * value)
                        ).astype(BF16)

        def back_step(step, source):
            for o in range(2):
                total = None
                for g in range(GROUP):
                    added = mm_t(
                        source[o, :, g * n : (g + 1) * n], row_tab[step * GROUP + g, o]
                    )
                    total = added if total is None else total + added
                grid[o] += total

        turns = pair_count // GROUP // 2
        fore_step(0, smear_a)

        def body(turn, carry):
            back_step(2 * turn, smear_a)
            fore_step(2 * turn + 1, smear_b)
            back_step(2 * turn + 1, smear_b)
            fore_step(2 * turn + 2, smear_a)
            return carry

        lax.fori_loop(0, turns - 1, body, 0)
        back_step(2 * turns - 2, smear_a)
        fore_step(2 * turns - 1, smear_b)
        back_step(2 * turns - 1, smear_b)

        for copy in copies:
            copy.wait_send()

        mark("turned")
        stack = []
        for p in range(2):
            low, high = grid[0, p * window : (p + 1) * window], grid[1, p * window : (p + 1) * window]
            stack += [
                low[:MARGIN] + high[half:], low[MARGIN:half],
                high[:MARGIN] + low[half:], high[MARGIN:half],
            ]
        turned = mm3(split(jnp.concatenate(stack, axis=0)), (right[0], right[1]))
        r_c, i_c = turned[:n, :half], turned[n:, :half]
        r_s, i_s = turned[:n, half:], turned[n:, half:]
        r_z, i_z = jnp.where(first_lane, 0.0, r_s), jnp.where(first_lane, 0.0, i_s)
        sides = [
            split(jnp.concatenate([r_c - i_z, i_c + r_z], axis=1)),
            split(jnp.concatenate(
                [jnp.where(first_lane, r_s, r_c + i_s), jnp.where(first_lane, i_s, i_c - r_s)], axis=1
            )),
        ]
        if it == 0:
            mark("mapwait")

            @pl.when(core != bit)
            def _():
                for b in range(blocks):
                    arrived(maps.at[:, b], map_recv.at[b])

            @pl.when(core == bit)
            def _():
                for b in direct:
                    arrived(maps.at[:, b], map_recv.at[b])

            for p in range(2):
                both = sum(
                    lax.dot_general(
                        x, perms[1], (((0,), (1,)), ((), ())), preferred_element_type=F32
                    )
                    for x in split(maps[p].reshape(n, n))
                )
                for q in range(2):
                    sens[p, q] = both[:, q * half : (q + 1) * half]

        mark("image")
        copies = []
        for q in range(2):
            w = mm3((back[0], back[1]), sides[q])
            c_r, c_i, s_r, s_i = w[:half, :half], w[:half, half:], w[half:, :half], w[half:, half:]
            z_r, z_i = jnp.where(first_row, 0.0, s_r), jnp.where(first_row, 0.0, s_i)
            low_r, low_i = c_r - z_i, c_i + z_r
            high_r = jnp.where(first_row, s_r, c_r + s_i)
            high_i = jnp.where(first_row, s_i, c_i - s_r)
            d_r = jnp.concatenate(
                [low_r, pltpu.roll(high_r[:groups], groups - 1, 0), high_r[groups:]], axis=0
            )
            d_i = jnp.concatenate(
                [low_i, pltpu.roll(high_i[:groups], groups - 1, 0), high_i[groups:]], axis=0
            )
            m_r, m_i = sens[0, q], sens[1, q]
            grads[slot, q, mine, 0] = m_r * d_r + m_i * d_i
            grads[slot, q, mine, 1] = m_r * d_i - m_i * d_r
            for d in range(1, coils):
                d_pair, d_core = d // CORES, d % CORES
                copy = pltpu.make_async_remote_copy(
                    src_ref=grads.at[slot, q, mine],
                    dst_ref=grads.at[slot, q, mine],
                    send_sem=grad_send.at[slot, q, d],
                    recv_sem=grad_recv.at[slot, q, mine],
                    device_id={
                        "coil": (coil + d_pair * CORES) % coils,
                        "spk": (core + d_core) % CORES,
                    },
                    device_id_type=MESH,
                )
                copy.start()
                copies.append(copy)

        coeff_of = []
        for q in range(2):
            mark("gradwait")
            for d in range(1, coils):
                d_pair, d_core = d // CORES, d % CORES
                other = (coil + d_pair * CORES) % coils // CORES * CORES + (core + d_core) % CORES
                pltpu.make_async_copy(
                    grads.at[slot, q, other], grads.at[slot, q, other], grad_recv.at[slot, q, other]
                ).wait()
            mark("shrink")
            summed = grads[slot, q, 0]
            for c in range(1, coils):
                summed = summed + grads[slot, q, c]
            target = -STEP_SIZE * jnp.concatenate([summed[0], summed[1]], axis=1)
            if it > 0:
                target = estimate[q] + target

            def piece(x, h, m):
                first = h * half + (m if h == 0 else (MEMBERS - m) % MEMBERS) * groups
                return x[first : first + groups]

            along = []
            for h in range(2):
                along += forward_haar([piece(target, h, m) for m in range(MEMBERS)])
            side = split(jnp.concatenate(along, axis=0))
            coeff_of.append(mm(side[0], haar[q, 0]) + mm(side[1], haar[q, 0]))
        for q in range(2):
            coeffs = coeff_of[q]
            shrunk = []
            for h in range(2):
                for k in range(MEMBERS):
                    first = h * half + k * groups
                    c_r = coeffs[first : first + groups, :half] * scales[k]
                    c_i = coeffs[first : first + groups, half:] * scales[k]
                    power = jnp.maximum(c_r * c_r + c_i * c_i, TINY)
                    factor = jnp.maximum(1.0 - limits[k] * lax.rsqrt(power), 0.0) * scales[k]
                    shrunk.append(jnp.concatenate([c_r * factor, c_i * factor], axis=1))
            side = split(jnp.concatenate(shrunk, axis=0))
            along = mm(side[0], haar[q, 1]) + mm(side[1], haar[q, 1])
            fresh = []
            for h in range(2):
                first = h * half
                members = inverse_haar(
                    [along[first + k * groups : first + (k + 1) * groups] for k in range(MEMBERS)]
                )
                placed = [None] * MEMBERS
                for m in range(MEMBERS):
                    placed[m if h == 0 else (MEMBERS - m) % MEMBERS] = members[m]
                fresh += placed
            fresh = jnp.concatenate(fresh, axis=0)
            estimate[q] = fresh
            if it < ITERS - 1:
                mark("fwd")
                e_r, e_i = fresh[:, :half], fresh[:, half:]
                m_r, m_i = sens[0, q], sens[1, q]
                seen = split(
                    jnp.concatenate([m_r * e_r - m_i * e_i, m_r * e_i + m_i * e_r], axis=1)
                )
                w = mm3((fore[0], fore[1]), seen)
                c_r, c_i, s_r, s_i = w[:half, :half], w[:half, half:], w[half:, :half], w[half:, half:]
                z_r, z_i = jnp.where(first_row, 0.0, s_r), jnp.where(first_row, 0.0, s_i)
                v = jnp.concatenate(
                    [
                        c_r + z_i, jnp.where(first_row, s_r, c_r - s_i),
                        c_i - z_r, jnp.where(first_row, s_i, c_i + s_r),
                    ],
                    axis=0,
                )
                half_h[:, q * half : (q + 1) * half], half_l[:, q * half : (q + 1) * half] = split(v)
        if it < ITERS - 1:
            mark("vfft")
            v = mm3((half_h[...], half_l[...]), (right[0], right[1]))
            r_c, i_c, r_s, i_s = v[:n, :half], v[n:, :half], v[:n, half:], v[n:, half:]
            r_z, i_z = jnp.where(first_lane, 0.0, r_s), jnp.where(first_lane, 0.0, i_s)
            whole = [
                jnp.concatenate([r_c + i_z, jnp.where(first_lane, r_s, r_c - i_s)], axis=1).astype(BF16),
                jnp.concatenate([i_c - r_z, jnp.where(first_lane, i_s, i_c + r_s)], axis=1).astype(BF16),
            ]
            for p in range(2):
                first = p * window
                kspace[0, first : first + window] = whole[p][:window]
                kspace[1, first : first + half] = whole[p][half:]
                kspace[1, first + half : first + window] = whole[p][:MARGIN]

    mark("out")
    take = lax.broadcasted_iota(jnp.int32, (rows, n), 0) + block * rows
    at = lax.broadcasted_iota(jnp.int32, (rows, n), 1)
    owner = jnp.where(at <= half, at, n + half - at)
    chosen = jnp.where(take == owner, 1.0, 0.0).astype(BF16)
    for p in range(2):
        mine_rows = jnp.concatenate([estimate[q, :, p * half : (p + 1) * half] for q in range(2)], axis=1)
        picked = sum(mm_t(chosen, x) for x in split(mine_rows))
        result = sum(mm(x, perms[0]) for x in split(picked))
        for t in range(n // LANES):
            out_ref[pl.ds(t * 2 + p, rows, stride=2 * n // LANES), :] = result[:, t * LANES : (t + 1) * LANES]

    @pl.when(core != bit)
    def _():
        for copy in inner:
            copy.wait_send()

    @pl.when(core == bit)
    def _():
        for _, there in data_hand + map_hand:
            there.wait_send()

    for copy in sends + copies:
        copy.wait_send()
    mark(None)


def local(coil_maps, kspace_data, interp_weights, sample_bins, spoke_count, thresholds):
    tiles, coils = lax.axis_size("tile"), lax.axis_size("coil")
    blocks = tiles * CORES
    rows, n = coil_maps.shape[1], coil_maps.shape[3]
    live = blocks * SPK_DEV // 2
    half = n // 2
    window = half + MARGIN
    consts = tables(n)
    vmem = pl.BlockSpec(memory_space=pltpu.VMEM)
    smem = pl.BlockSpec(memory_space=pltpu.SMEM)
    pair_count = live // 2
    dma = pltpu.SemaphoreType.DMA
    any_space = pl.BlockSpec(memory_space=pl.ANY)
    weights = jnp.transpose(interp_weights, (1, 0, 2))
    scratch = [pltpu.VMEM(c.shape, BF16) for c in consts] + [
            pltpu.VMEM(sample_bins.shape, jnp.int32),
            pltpu.VMEM(kspace_data.shape, BF16),
            pltpu.VMEM(coil_maps.shape, F32),
            pltpu.VMEM((FIELDS, SPK_DEV, n), BF16),
            pltpu.VMEM((blocks, FIELDS, SPK_DEV, n), BF16),
            pltpu.VMEM((SPK_DEV * 2, n), BF16),
            pltpu.VMEM((blocks, SPK_DEV * 2, n), BF16),
            pltpu.VMEM((2, rows, n), F32),
            pltpu.VMEM((2, blocks, rows, n), F32),
            pltpu.VMEM((2, 4 * TAPS, pair_count, n), F32),
            pltpu.VMEM((2, 3, pair_count, n), F32),
            pltpu.VMEM((pair_count, 2, n, n), BF16),
            pltpu.VMEM((pair_count, 2, window, n), BF16),
            pltpu.VMEM((2, 2 * window, n), BF16),
            pltpu.VMEM((2, 2 * window, n), F32),
            pltpu.VMEM((2, 2 * window, GROUP * n), BF16),
            pltpu.VMEM((2, 2 * window, GROUP * n), BF16),
            pltpu.VMEM((2 * n, n), BF16),
            pltpu.VMEM((2 * n, n), BF16),
            pltpu.VMEM((2, n, n), F32),
            pltpu.VMEM((2, 2, coils, 2, n, half), F32),
            pltpu.VMEM((2, 2, n, half), F32),
    ]
    out = pl.pallas_call(
        functools.partial(kernel, (n, tiles, coils, rows, live)),
        out_shape=jax.ShapeDtypeStruct((rows * 2 * n // LANES, LANES), F32),
        in_specs=[smem, smem] + [any_space] * (4 + len(consts)),
        out_specs=vmem,
        scratch_shapes=scratch + [
            dma((len(consts),)), dma((4,)),
            dma((blocks,)), dma((blocks,)), dma((2 + tiles + blocks,)), dma((blocks,)),
            dma((2 + tiles + blocks,)), dma((blocks,)),
            dma((2, 2, coils)), dma((2, 2, coils)),
        ],
        compiler_params=pltpu.CompilerParams(
            has_side_effects=True, collective_id=0, vmem_limit_bytes=VMEM_LIMIT
        ),
    )(thresholds, spoke_count, weights, sample_bins, kspace_data, coil_maps, *consts)
    out = out.reshape(rows, n // LANES, 2, LANES)
    return jnp.transpose(out, (0, 2, 1, 3)).reshape(rows, 2, n)


def solution(mesh):
    placed = (
        P("coil", ("grp", "tile", "spk"), None, None),
        P("coil", ("grp", "tile", "spk"), None, None),
        P(("grp", "tile", "spk"), None, None),
        P(("grp", "tile", "spk"), None),
        P(("grp", "tile", "spk")),
        P(),
    )
    return jax.shard_map(
        local,
        mesh=mesh,
        in_specs=placed,
        out_specs=P(("grp", "tile", "spk"), None, None),
        check_vma=False,
    )
```

```python
import functools
import math

import jax
import jax.numpy as jnp
import numpy as np
from jax import lax
from jax.experimental import pallas as pl
from jax.experimental.pallas import tpu as pltpu
from jax.sharding import PartitionSpec as P

SPK_DEV = 8
LEVELS = 3
MEMBERS = 2**LEVELS
ITERS = 4
CORES = 2
GROUP = 4
TAPS = 3
FIELDS = 8
MARGIN = 16
STEP_SIZE = 0.5
LANES = 128
TINY = 1e-30
VMEM_LIMIT = 60 * 1024 * 1024
F32 = jnp.float32
BF16 = jnp.bfloat16
MESH = pl.DeviceIdType.MESH

_scope = [None]


def mark(name):
    if _scope[0] is not None:
        _scope[0].__exit__(None, None, None)
        _scope[0] = None
    if name:
        _scope[0] = jax.named_scope(name)
        _scope[0].__enter__()


def split_np(table):
    table = np.ascontiguousarray(table).astype(np.float32)
    high = table.astype(jnp.bfloat16)
    low = (table - high.astype(np.float32)).astype(jnp.bfloat16)
    return high, low


def haar_signs(length, levels):
    mat = np.eye(length)
    for level in range(levels):
        span = length >> level
        half = span // 2
        step = np.eye(length)
        step[:span] = 0.0
        for i in range(half):
            step[i, 2 * i] = step[i, 2 * i + 1] = 1.0
            step[half + i, 2 * i] = 1.0
            step[half + i, 2 * i + 1] = -1.0
        mat = step @ mat
    return mat


def haar_labels(length, levels):
    label = np.ones((length,), np.int32)
    for level in range(1, levels + 1):
        label = label + (np.arange(length) < length >> level)
    return label


def mirror(first, n):
    second = (n - first) % n
    second[first == 0] = n // 2
    return np.concatenate([first, second])


def orders(n):
    half = n // 2
    by_lane = mirror(np.arange(half), n)
    edge = MARGIN // 2
    near = np.concatenate([np.arange(edge), np.arange(half - edge, half), np.arange(edge, half - edge)])
    by_freq = mirror(near, n)
    groups = half // MEMBERS
    member = np.arange(half) // groups
    group = np.arange(half) % groups
    low = MEMBERS * group + member
    high = n - MEMBERS * group - member
    high[:groups] = n - MEMBERS * (np.arange(groups) + 1)
    by_pixel = np.concatenate([low, high])
    return by_lane, by_freq, low, by_pixel


def tables(n):
    half = n // 2
    by_lane, by_freq, low, by_pixel = orders(n)
    phase = np.outer(np.arange(n), np.arange(n)) % n
    angle = phase * (2.0 * np.pi / n)
    cosine = np.cos(angle) / math.sqrt(n)
    sine = np.sin(angle) / math.sqrt(n)

    def folded(outs, ins):
        bottom = sine[outs][:, ins]
        bottom[outs == 0] = cosine[half][ins]
        return np.concatenate([cosine[outs][:, ins], bottom], axis=0)

    right = folded(np.arange(half), by_lane).T
    back = folded(low, by_freq)
    fore = folded(by_freq[:half], by_pixel)
    small = haar_signs(MEMBERS, LEVELS)
    chunk_haar = []
    for q in range(2):
        pixels = by_lane[q * half : (q + 1) * half]
        mat = np.zeros((half, half))
        group = pixels // MEMBERS - q * (half // MEMBERS)
        for k in range(MEMBERS):
            mat[group * MEMBERS + k, np.arange(half)] = small[k, pixels % MEMBERS]
        both = np.kron(np.eye(2), mat)
        chunk_haar.append((both.T, both))
    haar = np.stack([np.stack(pair) for pair in chunk_haar]).astype(jnp.bfloat16)
    windows = np.stack(
        [by_freq[: half + MARGIN], np.concatenate([by_freq[half:], by_freq[:MARGIN]])]
    )
    cell_u = np.repeat(by_lane[:, None], LANES, axis=1).astype(jnp.bfloat16)
    cell_v = np.repeat(windows[:, :, None], LANES, axis=2).astype(jnp.bfloat16)
    turn_s = np.zeros((n, n))
    turn_s[np.arange(n), by_pixel] = 1.0
    turn_r = np.zeros((n, n))
    turn_r[np.arange(n), by_lane] = 1.0
    perms = np.stack([turn_s, turn_r]).astype(jnp.bfloat16)
    return (
        np.stack(split_np(right)), np.stack(split_np(back)), np.stack(split_np(fore)),
        haar, cell_u, cell_v, perms,
    )


def split(x):
    high = x.astype(BF16)
    return high, (x - high.astype(F32)).astype(BF16)


def mm(a, b):
    return jnp.dot(a, b, preferred_element_type=F32)


def mm_t(a, b):
    return lax.dot_general(a, b, (((1,), (1,)), ((), ())), preferred_element_type=F32)


def mm3(a, b):
    return mm(a[0], b[0]) + (mm(a[0], b[1]) + mm(a[1], b[0]))


def forward_haar(x):
    sums = [x[2 * i] + x[2 * i + 1] for i in range(4)]
    out = [None] * 4 + [x[2 * i] - x[2 * i + 1] for i in range(4)]
    pair = [sums[0] + sums[1], sums[2] + sums[3]]
    out[2], out[3] = sums[0] - sums[1], sums[2] - sums[3]
    out[0], out[1] = pair[0] + pair[1], pair[0] - pair[1]
    return out


def inverse_haar(c):
    pair = [c[0] + c[1], c[0] - c[1]]
    sums = [pair[0] + c[2], pair[0] - c[2], pair[1] + c[3], pair[1] - c[3]]
    out = []
    for i in range(4):
        out += [sums[i] + c[4 + i], sums[i] - c[4 + i]]
    return out


def kernel(
    dims,
    thr_ref, count_ref, weight_hbm, bins_hbm, data_hbm, map_hbm,
    right_hbm, back_hbm, fore_hbm, haar_hbm, cell_u_hbm, cell_v_hbm, perm_hbm,
    out_ref,
    right, back, fore, haar, cell_u, cell_v, perms,
    bins_ref, data_ref, map_ref, meta_mine, meta_all, data_mine, data_all, map_mine, maps,
    pairs, pair_data, row_tab, col_tab, kspace, grid, smear_a, smear_b,
    half_h, half_l, estimate, grads, sens,
    const_sem, arg_sem, meta_send, meta_recv, data_send, data_recv, map_send, map_recv, grad_send, grad_recv,
):
    n, tiles, coils, rows, live = dims
    half = n // 2
    window = half + MARGIN
    blocks = tiles * CORES
    slots = blocks * SPK_DEV
    pair_count = live // 2
    coil, tile, core = lax.axis_index("coil"), lax.axis_index("tile"), lax.axis_index("spk")
    pair, bit = coil // CORES, coil % CORES
    block = tile * CORES + core
    mine = pair * CORES + core

    def toggled(value, d):
        step = 1
        while step <= d:
            if d & step:
                value = value + step - 2 * step * (value // step % 2)
            step *= 2
        return value

    mark("start")
    barrier = pltpu.get_barrier_semaphore()
    peers = [
        (d_bit, d_tile, d_core)
        for d_bit in range(CORES)
        for d_tile in range(tiles)
        for d_core in range(CORES)
        if (d_tile > 0 and d_bit == 0) or (d_tile < 2 and d_tile + d_bit + d_core > 0)
    ]
    for d_bit, d_tile, d_core in peers:
        pl.semaphore_signal(
            barrier,
            inc=1,
            device_id={
                "coil": pair * CORES + (bit + d_bit) % CORES,
                "tile": toggled(tile, d_tile),
                "spk": (core + d_core) % CORES,
            },
            device_id_type=MESH,
        )
    for d in range(CORES, coils):
        pl.semaphore_signal(
            barrier,
            inc=1,
            device_id={
                "coil": (coil + d // CORES * CORES) % coils,
                "spk": (core + d % CORES) % CORES,
            },
            device_id_type=MESH,
        )
    arg_copies = []
    for k, (src, dst) in enumerate((
        (bins_hbm, bins_ref), (weight_hbm, meta_mine.at[: 2 * TAPS]),
        (data_hbm, data_ref), (map_hbm, map_ref),
    )):
        copy = pltpu.make_async_copy(src, dst, arg_sem.at[k])
        copy.start()
        arg_copies.append(copy)
    const_copies = []
    for k, (src, dst) in enumerate((
        (perm_hbm, perms), (cell_u_hbm, cell_u), (cell_v_hbm, cell_v), (right_hbm, right),
        (back_hbm, back), (haar_hbm, haar), (fore_hbm, fore),
    )):
        copy = pltpu.make_async_copy(src, dst, const_sem.at[k])
        copy.start()
        const_copies.append(copy)

    mark("prep")
    for copy in arg_copies:
        copy.wait()
    alive = lax.broadcasted_iota(jnp.int32, (SPK_DEV, n), 0) < count_ref[0]
    bins = bins_ref[...]
    row_of = jnp.where(alive, bins // n, -1).astype(F32)
    col_of = (bins % n).astype(F32)
    meta_mine[2 * TAPS] = row_of.astype(BF16)
    meta_mine[2 * TAPS + 1] = col_of.astype(BF16)
    data_wide = data_ref[0].astype(F32)
    data_mine[...] = jnp.concatenate([data_wide[:, 0], data_wide[:, 1]], axis=0).astype(BF16)
    mark("barrier")
    pl.semaphore_wait(barrier, len(peers) + coils - CORES)

    mark("issue")
    sends = []
    near = [toggled(tile, d) for d in range(tiles)]
    far_first = list(range(tiles // 2, tiles)) + list(range(1, tiles // 2))

    def send(src, dst, s_sem, r_sem, target):
        copy = pltpu.make_async_remote_copy(
            src_ref=src, dst_ref=dst, send_sem=s_sem, recv_sem=r_sem,
            device_id=target, device_id_type=MESH,
        )
        copy.start()
        return copy

    for d in far_first:
        sends.append(send(
            meta_mine, meta_all.at[block], meta_send.at[d], meta_recv.at[block], {"tile": near[d]}
        ))
    sends.append(send(
        meta_mine, meta_all.at[block], meta_send.at[0], meta_recv.at[block], {"spk": 1 - core}
    ))
    inner = []
    across = pair * CORES + 1 - bit
    routes = [{"coil": across, "spk": bit}, {"tile": near[1], "spk": bit},
              {"coil": across, "tile": near[1], "spk": bit}]
    far = [d for d in far_first if d > 1]
    even = [d for d in far if d % 2 == 0]

    def outward(distances):
        return [{"tile": near[d], "spk": bit} for d in distances]

    def spread(src, dst, s_sem, r_sem, targets):
        for k, target in enumerate(targets):
            sends.append(send(src, dst, s_sem.at[1 + k], r_sem, target))
        local_copy = pltpu.make_async_copy(src, dst, r_sem)
        inner_copy = pltpu.make_async_remote_copy(
            src_ref=src, dst_ref=dst, send_sem=s_sem.at[0], recv_sem=r_sem,
            device_id={"spk": 1 - core}, device_id_type=MESH,
        )
        inner.append(inner_copy)

        @pl.when(core == bit)
        def _():
            local_copy.start()

        @pl.when(core != bit)
        def _():
            inner_copy.start()

    spread(data_mine, data_all.at[block], data_send, data_recv.at[block], routes + outward(far))
    const_copies[0].wait()
    for p in range(2):
        map_mine[p] = sum(mm_t(x, perms[0]) for x in split(map_ref[0, :, p, :]))
    spread(map_mine, maps.at[:, block], map_send, map_recv.at[block], routes[:1] + outward(even) + routes[1:])

    def arrived(ref, sem):
        pltpu.make_async_copy(ref, ref, sem).wait()

    beyond = [{"coil": across}, {"tile": near[1]}, {"coil": across, "tile": near[1]}]

    def hand_over(ref, s_sem, first, r_sem, targets):
        return (
            pltpu.make_async_copy(ref, ref, r_sem),
            [
                pltpu.make_async_remote_copy(
                    src_ref=ref, dst_ref=ref, send_sem=s_sem.at[first + k], recv_sem=r_sem,
                    device_id=target, device_id_type=MESH,
                )
                for k, target in enumerate(targets)
            ],
        )

    map_hand, data_hand = [], []
    for d in far:
        for c in range(CORES):
            b = near[d] * CORES + c
            data_hand.append(hand_over(
                data_all.at[b], data_send, 2 + tiles + len(data_hand), data_recv.at[b], beyond[:1]
            ))
            if d in even:
                map_hand.append(hand_over(
                    maps.at[:, b], map_send, 2 + tiles + 3 * len(map_hand), map_recv.at[b], beyond
                ))

    def pass_on(hands):
        @pl.when(core == bit)
        def _():
            for here, there in hands:
                here.wait()
                for copy in there:
                    copy.start()

    mark("metawait")
    for copy in const_copies[1:]:
        copy.wait()
    meta_all[block] = meta_mine[...]
    for d in range(1, tiles):
        b = near[d] * CORES + core
        arrived(meta_all.at[b], meta_recv.at[b])
        sends.append(send(
            meta_all.at[b], meta_all.at[b], meta_send.at[tiles + d], meta_recv.at[b], {"spk": 1 - core}
        ))
    for d in range(tiles):
        b = near[d] * CORES + 1 - core
        arrived(meta_all.at[b], meta_recv.at[b])

    mark("rank")
    whole = [meta_all[b].reshape(FIELDS * SPK_DEV, n).astype(F32) for b in range(blocks)]

    def field(m):
        return jnp.concatenate([w[m * SPK_DEV : (m + 1) * SPK_DEV] for w in whole], axis=0)

    rows_all = field(2 * TAPS)
    up = lax.broadcasted_iota(jnp.int32, (slots, slots), 0)
    across = lax.broadcasted_iota(jnp.int32, (slots, slots), 1)
    flag = jnp.where(rows_all[:, :LANES] >= 0.0, 1.0 / LANES, 0.0)
    flags = mm_t(jnp.ones((live, LANES), BF16), flag.astype(BF16)).astype(BF16)
    rank = mm(flags, jnp.where(up < across, 1.0, 0.0).astype(BF16))
    here = lax.broadcasted_iota(jnp.int32, (live, slots), 0).astype(F32)
    hit = (flags.astype(F32) > 0.5) & (rank == here)
    pick = jnp.where(hit, 1.0, 0.0).astype(BF16)
    comp = [mm(pick, (rows_all if m == 2 * TAPS else field(m)).astype(BF16)) for m in range(FIELDS)]
    first_low = jnp.broadcast_to(comp[2 * TAPS + 1][:, 1:2], (live, half)) < half

    def halves(x):
        low = jnp.where(first_low, x[:, :half], x[:, half:])
        high = jnp.where(first_low, x[:, half:], x[:, :half])
        return [jnp.concatenate([v[:pair_count], v[pair_count:]], axis=1) for v in (low, high)]

    for m in range(2 * TAPS):
        for o, value in enumerate(halves(comp[m])):
            pairs[o, m] = value
    for m, centre in ((2 * TAPS, comp[2 * TAPS]), (3 * TAPS, comp[2 * TAPS + 1])):
        for t in range(TAPS):
            tap = (centre.astype(jnp.int32) + (t - 1)) & (n - 1)
            for o, value in enumerate(halves(tap.astype(F32))):
                pairs[o, m + t] = value

    mark("build")

    def build(i, carry):
        def table(cells, m, o):
            def part(k):
                return jnp.broadcast_to(pairs[o, k, pl.ds(i, 1), :].astype(BF16), cells.shape)

            zero = jnp.zeros(cells.shape, BF16)
            return jnp.where(
                cells == part(2 * TAPS + m), part(m),
                jnp.where(
                    cells == part(2 * TAPS + m + 1), part(m + 1),
                    jnp.where(cells == part(2 * TAPS + m + 2), part(m + 2), zero),
                ),
            )

        for o in range(2):
            cells = jnp.concatenate([cell_u[...]] * (n // LANES), axis=1)
            row_tab[i, o] = table(cells, 0, o)
            cells = jnp.concatenate([cell_v[o]] * (n // LANES), axis=1)
            col_tab[i, o] = table(cells, TAPS, o)
        return carry

    lax.fori_loop(0, pair_count // 2, build, 0)

    mark("pass")
    pass_on(data_hand)
    pass_on(map_hand)
    direct = [near[d] * CORES + c for d in range(2) for c in range(CORES)]
    last_maps = [near[d] * CORES + c for d in [0] + list(range(1, tiles, 2)) for c in range(CORES)]

    @pl.when(core == bit)
    def _():
        for b in direct:
            arrived(data_all.at[b], data_recv.at[b])

    mark("build2")
    lax.fori_loop(pair_count // 2, pair_count, build, 0)

    mark("datawait")

    @pl.when(core != bit)
    def _():
        for b in range(blocks):
            arrived(data_all.at[b], data_recv.at[b])

    offset = jnp.abs(lax.broadcasted_iota(jnp.int32, (live, n), 1) - half).astype(F32)
    density = (offset + 0.5) * (n / (3.0 * n * live))
    for o, value in enumerate(halves(density)):
        pair_data[o, 2] = value
    every = data_all[...]
    for p in range(2):
        samples = jnp.concatenate(
            [every[b].astype(F32)[p * SPK_DEV : (p + 1) * SPK_DEV] for b in range(blocks)], axis=0
        )
        for o, value in enumerate(halves(mm(pick, samples.astype(BF16)))):
            pair_data[o, p] = value

    first_lane = lax.broadcasted_iota(jnp.int32, (n, half), 1) == 0
    first_row = lax.broadcasted_iota(jnp.int32, (half, half), 0) == 0
    groups = half // MEMBERS
    label = haar_labels(MEMBERS, LEVELS)
    lane = lax.broadcasted_iota(jnp.int32, (1, half), 1) % MEMBERS
    lane_label = jnp.ones((1, half), jnp.int32)
    for level in range(1, LEVELS + 1):
        lane_label = lane_label + jnp.where(lane < MEMBERS >> level, 1, 0)

    def norm_of(k):
        return 1.0 / math.sqrt((haar_signs(MEMBERS, LEVELS)[k] ** 2).sum())

    lane_norm = jnp.zeros((1, half), F32)
    for k in range(MEMBERS):
        lane_norm = jnp.where(lane == k, norm_of(k), lane_norm)
    limits, scales = [], []
    for k in range(MEMBERS):
        band = jnp.minimum(lane_label, int(label[k]))
        limit = jnp.zeros((1, half), F32)
        for level in range(LEVELS):
            limit = jnp.where(band == level + 1, thr_ref[level], limit)
        limits.append(limit)
        scales.append(lane_norm * norm_of(k))
    steps_of = [-STEP_SIZE * scale for scale in scales]
    own_half = block // (blocks // 2)

    copies = []
    for it in range(ITERS):
        slot = it % 2
        mark("spokes")
        grid[...] = jnp.zeros_like(grid)

        def fore_step(step, into, it=it):
            for g in range(GROUP):
                i = step * GROUP + g
                for o in range(2):
                    col = col_tab[i, o].astype(F32)
                    dens = pair_data[o, 2, pl.ds(i, 1), :]
                    seen = mm(kspace[o], row_tab[i, o]) if it > 0 else None
                    for p in range(2):
                        value = -pair_data[o, p, pl.ds(i, 1), :]
                        if it > 0:
                            value = value + jnp.sum(
                                seen[p * window : (p + 1) * window] * col, axis=0, keepdims=True
                            )
                        into[o, p * window : (p + 1) * window, g * n : (g + 1) * n] = (
                            col * (dens * value)
                        ).astype(BF16)

        def back_step(step, source):
            for o in range(2):
                total = None
                for g in range(GROUP):
                    added = mm_t(
                        source[o, :, g * n : (g + 1) * n], row_tab[step * GROUP + g, o]
                    )
                    total = added if total is None else total + added
                grid[o] += total

        turns = pair_count // GROUP // 2
        fore_step(0, smear_a)

        def body(turn, carry):
            back_step(2 * turn, smear_a)
            fore_step(2 * turn + 1, smear_b)
            back_step(2 * turn + 1, smear_b)
            fore_step(2 * turn + 2, smear_a)
            return carry

        lax.fori_loop(0, turns - 1, body, 0)
        back_step(2 * turns - 2, smear_a)
        fore_step(2 * turns - 1, smear_b)
        back_step(2 * turns - 1, smear_b)

        for copy in copies:
            copy.wait_send()

        mark("turned")
        stack = []
        for p in range(2):
            low, high = grid[0, p * window : (p + 1) * window], grid[1, p * window : (p + 1) * window]
            stack += [
                low[:MARGIN] + high[half:], low[MARGIN:half],
                high[:MARGIN] + low[half:], high[MARGIN:half],
            ]
        turned = mm3(split(jnp.concatenate(stack, axis=0)), (right[0], right[1]))
        r_c, i_c = turned[:n, :half], turned[n:, :half]
        r_s, i_s = turned[:n, half:], turned[n:, half:]
        r_z, i_z = jnp.where(first_lane, 0.0, r_s), jnp.where(first_lane, 0.0, i_s)
        sides = [
            split(jnp.concatenate([r_c - i_z, i_c + r_z], axis=1)),
            split(jnp.concatenate(
                [jnp.where(first_lane, r_s, r_c + i_s), jnp.where(first_lane, i_s, i_c - r_s)], axis=1
            )),
        ]
        if it == 0:
            mark("mapwait")

            @pl.when(core != bit)
            def _():
                for b in range(blocks):
                    arrived(maps.at[:, b], map_recv.at[b])

            @pl.when(core == bit)
            def _():
                for b in last_maps:
                    arrived(maps.at[:, b], map_recv.at[b])

            for p in range(2):
                both = sum(
                    lax.dot_general(
                        x, perms[1], (((0,), (1,)), ((), ())), preferred_element_type=F32
                    )
                    for x in split(maps[p].reshape(n, n))
                )
                for q in range(2):
                    sens[p, q] = both[:, q * half : (q + 1) * half]

        mark("image")
        last = it == ITERS - 1
        chunks = [own_half] if last else [0, 1]
        if last:
            sides = [[jnp.where(own_half == 0, a, b) for a, b in zip(*sides)]]
        copies = []
        for q, side in zip(chunks, sides):
            w = mm3((back[0], back[1]), side)
            c_r, c_i, s_r, s_i = w[:half, :half], w[:half, half:], w[half:, :half], w[half:, half:]
            z_r, z_i = jnp.where(first_row, 0.0, s_r), jnp.where(first_row, 0.0, s_i)
            low_r, low_i = c_r - z_i, c_i + z_r
            high_r = jnp.where(first_row, s_r, c_r + s_i)
            high_i = jnp.where(first_row, s_i, c_i - s_r)
            d_r = jnp.concatenate(
                [low_r, pltpu.roll(high_r[:groups], groups - 1, 0), high_r[groups:]], axis=0
            )
            d_i = jnp.concatenate(
                [low_i, pltpu.roll(high_i[:groups], groups - 1, 0), high_i[groups:]], axis=0
            )
            m_r, m_i = sens[0, q], sens[1, q]
            combined = jnp.concatenate([m_r * d_r + m_i * d_i, m_r * d_i - m_i * d_r], axis=1)

            def piece(x, h, m):
                first = h * half + (m if h == 0 else (MEMBERS - m) % MEMBERS) * groups
                return x[first : first + groups]

            along = []
            for h in range(2):
                along += forward_haar([piece(combined, h, m) for m in range(MEMBERS)])
            side = split(jnp.concatenate(along, axis=0))
            grads[slot, q, mine] = mm(side[0], haar[q, 0]) + mm(side[1], haar[q, 0])
            for d in range(1, coils):
                d_pair, d_core = d // CORES, d % CORES
                copy = pltpu.make_async_remote_copy(
                    src_ref=grads.at[slot, q, mine],
                    dst_ref=grads.at[slot, q, mine],
                    send_sem=grad_send.at[slot, q, d],
                    recv_sem=grad_recv.at[slot, q, mine],
                    device_id={
                        "coil": (coil + d_pair * CORES) % coils,
                        "spk": (core + d_core) % CORES,
                    },
                    device_id_type=MESH,
                )
                copy.start()
                copies.append(copy)

        for q in chunks:
            mark("gradwait")
            for d in range(1, coils):
                d_pair, d_core = d // CORES, d % CORES
                other = (coil + d_pair * CORES) % coils // CORES * CORES + (core + d_core) % CORES
                pltpu.make_async_copy(
                    grads.at[slot, q, other], grads.at[slot, q, other], grad_recv.at[slot, q, other]
                ).wait()
            mark("shrink")
            summed = grads[slot, q, 0]
            for c in range(1, coils):
                summed = summed + grads[slot, q, c]
            shrunk = []
            for h in range(2):
                for k in range(MEMBERS):
                    at = slice(h * half + k * groups, h * half + (k + 1) * groups)
                    c_r = summed[at, :half] * steps_of[k]
                    c_i = summed[at, half:] * steps_of[k]
                    if it > 0:
                        c_r, c_i = estimate[q, at, :half] + c_r, estimate[q, at, half:] + c_i
                    power = jnp.maximum(c_r * c_r + c_i * c_i, TINY)
                    factor = jnp.maximum(1.0 - limits[k] * lax.rsqrt(power), 0.0)
                    c_r, c_i = c_r * factor, c_i * factor
                    if not last:
                        estimate[q, at, :half], estimate[q, at, half:] = c_r, c_i
                    shrunk.append(jnp.concatenate([c_r * scales[k], c_i * scales[k]], axis=1))
            side = split(jnp.concatenate(shrunk, axis=0))
            along = mm(side[0], haar[q, 1]) + mm(side[1], haar[q, 1])
            fresh = []
            for h in range(2):
                first = h * half
                members = inverse_haar(
                    [along[first + k * groups : first + (k + 1) * groups] for k in range(MEMBERS)]
                )
                placed = [None] * MEMBERS
                for m in range(MEMBERS):
                    placed[m if h == 0 else (MEMBERS - m) % MEMBERS] = members[m]
                fresh += placed
            fresh = jnp.concatenate(fresh, axis=0)
            if it < ITERS - 1:
                mark("fwd")
                e_r, e_i = fresh[:, :half], fresh[:, half:]
                m_r, m_i = sens[0, q], sens[1, q]
                seen = split(
                    jnp.concatenate([m_r * e_r - m_i * e_i, m_r * e_i + m_i * e_r], axis=1)
                )
                w = mm3((fore[0], fore[1]), seen)
                c_r, c_i, s_r, s_i = w[:half, :half], w[:half, half:], w[half:, :half], w[half:, half:]
                z_r, z_i = jnp.where(first_row, 0.0, s_r), jnp.where(first_row, 0.0, s_i)
                v = jnp.concatenate(
                    [
                        c_r + z_i, jnp.where(first_row, s_r, c_r - s_i),
                        c_i - z_r, jnp.where(first_row, s_i, c_i + s_r),
                    ],
                    axis=0,
                )
                half_h[:, q * half : (q + 1) * half], half_l[:, q * half : (q + 1) * half] = split(v)
        if it < ITERS - 1:
            mark("vfft")
            v = mm3((half_h[...], half_l[...]), (right[0], right[1]))
            r_c, i_c, r_s, i_s = v[:n, :half], v[n:, :half], v[:n, half:], v[n:, half:]
            r_z, i_z = jnp.where(first_lane, 0.0, r_s), jnp.where(first_lane, 0.0, i_s)
            whole = [
                jnp.concatenate([r_c + i_z, jnp.where(first_lane, r_s, r_c - i_s)], axis=1).astype(BF16),
                jnp.concatenate([i_c - r_z, jnp.where(first_lane, i_s, i_c + r_s)], axis=1).astype(BF16),
            ]
            for p in range(2):
                first = p * window
                kspace[0, first : first + window] = whole[p][:window]
                kspace[1, first : first + half] = whole[p][half:]
                kspace[1, first + half : first + window] = whole[p][:MARGIN]

    mark("out")
    take = lax.broadcasted_iota(jnp.int32, (rows, half), 0) + block * rows
    at = lax.broadcasted_iota(jnp.int32, (rows, half), 1)
    owner = jnp.where(own_half == 0, at, jnp.where(at == 0, half, n - at))
    chosen = jnp.where(take == owner, 1.0, 0.0).astype(BF16)
    for p in range(2):
        picked = sum(mm_t(chosen, x) for x in split(fresh[:, p * half : (p + 1) * half]))
        result = sum(mm(x, perms[0]) for x in split(picked))
        for t in range(n // LANES):
            out_ref[pl.ds(t * 2 + p, rows, stride=2 * n // LANES), :] = result[:, t * LANES : (t + 1) * LANES]

    @pl.when(core != bit)
    def _():
        for copy in inner:
            copy.wait_send()

    @pl.when(core == bit)
    def _():
        for _, there in data_hand + map_hand:
            for copy in there:
                copy.wait_send()

    for copy in sends + copies:
        copy.wait_send()
    mark(None)


def local(coil_maps, kspace_data, interp_weights, sample_bins, spoke_count, thresholds):
    tiles, coils = lax.axis_size("tile"), lax.axis_size("coil")
    blocks = tiles * CORES
    rows, n = coil_maps.shape[1], coil_maps.shape[3]
    live = blocks * SPK_DEV // 2
    half = n // 2
    window = half + MARGIN
    consts = tables(n)
    vmem = pl.BlockSpec(memory_space=pltpu.VMEM)
    smem = pl.BlockSpec(memory_space=pltpu.SMEM)
    pair_count = live // 2
    dma = pltpu.SemaphoreType.DMA
    any_space = pl.BlockSpec(memory_space=pl.ANY)
    weights = jnp.transpose(interp_weights, (1, 0, 2))
    scratch = [pltpu.VMEM(c.shape, BF16) for c in consts] + [
            pltpu.VMEM(sample_bins.shape, jnp.int32),
            pltpu.VMEM(kspace_data.shape, BF16),
            pltpu.VMEM(coil_maps.shape, F32),
            pltpu.VMEM((FIELDS, SPK_DEV, n), BF16),
            pltpu.VMEM((blocks, FIELDS, SPK_DEV, n), BF16),
            pltpu.VMEM((SPK_DEV * 2, n), BF16),
            pltpu.VMEM((blocks, SPK_DEV * 2, n), BF16),
            pltpu.VMEM((2, rows, n), F32),
            pltpu.VMEM((2, blocks, rows, n), F32),
            pltpu.VMEM((2, 4 * TAPS, pair_count, n), F32),
            pltpu.VMEM((2, 3, pair_count, n), F32),
            pltpu.VMEM((pair_count, 2, n, n), BF16),
            pltpu.VMEM((pair_count, 2, window, n), BF16),
            pltpu.VMEM((2, 2 * window, n), BF16),
            pltpu.VMEM((2, 2 * window, n), F32),
            pltpu.VMEM((2, 2 * window, GROUP * n), BF16),
            pltpu.VMEM((2, 2 * window, GROUP * n), BF16),
            pltpu.VMEM((2 * n, n), BF16),
            pltpu.VMEM((2 * n, n), BF16),
            pltpu.VMEM((2, n, n), F32),
            pltpu.VMEM((2, 2, coils, n, n), F32),
            pltpu.VMEM((2, 2, n, half), F32),
    ]
    out = pl.pallas_call(
        functools.partial(kernel, (n, tiles, coils, rows, live)),
        out_shape=jax.ShapeDtypeStruct((rows * 2 * n // LANES, LANES), F32),
        in_specs=[smem, smem] + [any_space] * (4 + len(consts)),
        out_specs=vmem,
        scratch_shapes=scratch + [
            dma((len(consts),)), dma((4,)),
            dma((blocks,)), dma((blocks,)), dma((2 + tiles + 3 * blocks,)), dma((blocks,)),
            dma((2 + tiles + 3 * blocks,)), dma((blocks,)),
            dma((2, 2, coils)), dma((2, 2, coils)),
        ],
        compiler_params=pltpu.CompilerParams(
            has_side_effects=True, collective_id=0, vmem_limit_bytes=VMEM_LIMIT
        ),
    )(thresholds, spoke_count, weights, sample_bins, kspace_data, coil_maps, *consts)
    out = out.reshape(rows, n // LANES, 2, LANES)
    return jnp.transpose(out, (0, 2, 1, 3)).reshape(rows, 2, n)


def solution(mesh):
    placed = (
        P("coil", ("grp", "tile", "spk"), None, None),
        P("coil", ("grp", "tile", "spk"), None, None),
        P(("grp", "tile", "spk"), None, None),
        P(("grp", "tile", "spk"), None),
        P(("grp", "tile", "spk")),
        P(),
    )
    return jax.shard_map(
        local,
        mesh=mesh,
        in_specs=placed,
        out_specs=P(("grp", "tile", "spk"), None, None),
        check_vma=False,
    )
```

```python
import functools
import math

import jax
import jax.numpy as jnp
import numpy as np
from jax import lax
from jax.experimental import pallas as pl
from jax.experimental.pallas import tpu as pltpu
from jax.sharding import PartitionSpec as P

SPK_DEV = 8
LEVELS = 3
MEMBERS = 2**LEVELS
ITERS = 4
CORES = 2
GROUP = 4
TAPS = 3
FIELDS = 8
MARGIN = 16
STEP_SIZE = 0.5
LANES = 128
TINY = 1e-30
VMEM_LIMIT = 60 * 1024 * 1024
F32 = jnp.float32
BF16 = jnp.bfloat16
MESH = pl.DeviceIdType.MESH

_scope = [None]


def mark(name):
    if _scope[0] is not None:
        _scope[0].__exit__(None, None, None)
        _scope[0] = None
    if name:
        _scope[0] = jax.named_scope(name)
        _scope[0].__enter__()


def split_np(table):
    table = np.ascontiguousarray(table).astype(np.float32)
    high = table.astype(jnp.bfloat16)
    low = (table - high.astype(np.float32)).astype(jnp.bfloat16)
    return high, low


def haar_signs(length, levels):
    mat = np.eye(length)
    for level in range(levels):
        span = length >> level
        half = span // 2
        step = np.eye(length)
        step[:span] = 0.0
        for i in range(half):
            step[i, 2 * i] = step[i, 2 * i + 1] = 1.0
            step[half + i, 2 * i] = 1.0
            step[half + i, 2 * i + 1] = -1.0
        mat = step @ mat
    return mat


def haar_labels(length, levels):
    label = np.ones((length,), np.int32)
    for level in range(1, levels + 1):
        label = label + (np.arange(length) < length >> level)
    return label


def mirror(first, n):
    second = (n - first) % n
    second[first == 0] = n // 2
    return np.concatenate([first, second])


def orders(n):
    half = n // 2
    by_lane = mirror(np.arange(half), n)
    edge = MARGIN // 2
    near = np.concatenate([np.arange(edge), np.arange(half - edge, half), np.arange(edge, half - edge)])
    by_freq = mirror(near, n)
    groups = half // MEMBERS
    member = np.arange(half) // groups
    group = np.arange(half) % groups
    low = MEMBERS * group + member
    high = n - MEMBERS * group - member
    high[:groups] = n - MEMBERS * (np.arange(groups) + 1)
    by_pixel = np.concatenate([low, high])
    return by_lane, by_freq, low, by_pixel


def tables(n):
    half = n // 2
    by_lane, by_freq, low, by_pixel = orders(n)
    phase = np.outer(np.arange(n), np.arange(n)) % n
    angle = phase * (2.0 * np.pi / n)
    cosine = np.cos(angle) / math.sqrt(n)
    sine = np.sin(angle) / math.sqrt(n)

    def folded(outs, ins):
        bottom = sine[outs][:, ins]
        bottom[outs == 0] = cosine[half][ins]
        return np.concatenate([cosine[outs][:, ins], bottom], axis=0)

    right = folded(np.arange(half), by_lane).T
    back = folded(low, by_freq)
    fore = folded(by_freq[:half], by_pixel)
    small = haar_signs(MEMBERS, LEVELS)
    chunk_haar = []
    for q in range(2):
        pixels = by_lane[q * half : (q + 1) * half]
        mat = np.zeros((half, half))
        group = pixels // MEMBERS - q * (half // MEMBERS)
        for k in range(MEMBERS):
            mat[group * MEMBERS + k, np.arange(half)] = small[k, pixels % MEMBERS]
        both = np.kron(np.eye(2), mat)
        chunk_haar.append((both.T, both))
    haar = np.stack([np.stack(pair) for pair in chunk_haar]).astype(jnp.bfloat16)
    windows = np.stack(
        [by_freq[: half + MARGIN], np.concatenate([by_freq[half:], by_freq[:MARGIN]])]
    )
    cell_u = np.repeat(by_lane[:, None], LANES, axis=1).astype(jnp.bfloat16)
    cell_v = np.repeat(windows[:, :, None], LANES, axis=2).astype(jnp.bfloat16)
    turn_s = np.zeros((n, n))
    turn_s[np.arange(n), by_pixel] = 1.0
    turn_r = np.zeros((n, n))
    turn_r[np.arange(n), by_lane] = 1.0
    perms = np.stack([turn_s, turn_r]).astype(jnp.bfloat16)
    return (
        np.stack(split_np(right)), np.stack(split_np(back)), np.stack(split_np(fore)),
        haar, cell_u, cell_v, perms,
    )


def split(x):
    high = x.astype(BF16)
    return high, (x - high.astype(F32)).astype(BF16)


def mm(a, b):
    return jnp.dot(a, b, preferred_element_type=F32)


def mm_t(a, b):
    return lax.dot_general(a, b, (((1,), (1,)), ((), ())), preferred_element_type=F32)


def mm3(a, b):
    return mm(a[0], b[0]) + (mm(a[0], b[1]) + mm(a[1], b[0]))


def forward_haar(x):
    sums = [x[2 * i] + x[2 * i + 1] for i in range(4)]
    out = [None] * 4 + [x[2 * i] - x[2 * i + 1] for i in range(4)]
    pair = [sums[0] + sums[1], sums[2] + sums[3]]
    out[2], out[3] = sums[0] - sums[1], sums[2] - sums[3]
    out[0], out[1] = pair[0] + pair[1], pair[0] - pair[1]
    return out


def inverse_haar(c):
    pair = [c[0] + c[1], c[0] - c[1]]
    sums = [pair[0] + c[2], pair[0] - c[2], pair[1] + c[3], pair[1] - c[3]]
    out = []
    for i in range(4):
        out += [sums[i] + c[4 + i], sums[i] - c[4 + i]]
    return out


def kernel(
    dims,
    thr_ref, count_ref, weight_hbm, bins_hbm, data_hbm, map_hbm,
    right_hbm, back_hbm, fore_hbm, haar_hbm, cell_u_hbm, cell_v_hbm, perm_hbm,
    out_ref,
    right, back, fore, haar, cell_u, cell_v, perms,
    bins_ref, data_ref, map_ref, meta_mine, meta_all, data_mine, data_all, map_mine, maps,
    pairs, pair_data, row_tab, col_tab, kspace, grid, smear_a, smear_b,
    half_h, half_l, estimate, grads, sens,
    const_sem, arg_sem, meta_send, meta_recv, data_send, data_recv, map_send, map_recv, grad_send, grad_recv,
):
    n, tiles, coils, rows, live = dims
    half = n // 2
    window = half + MARGIN
    blocks = tiles * CORES
    slots = blocks * SPK_DEV
    pair_count = live // 2
    coil, tile, core = lax.axis_index("coil"), lax.axis_index("tile"), lax.axis_index("spk")
    pair, bit = coil // CORES, coil % CORES
    block = tile * CORES + core
    mine = pair * CORES + core

    def toggled(value, d):
        step = 1
        while step <= d:
            if d & step:
                value = value + step - 2 * step * (value // step % 2)
            step *= 2
        return value

    mark("start")
    arg_copies = []
    for k, (src, dst) in enumerate((
        (bins_hbm, bins_ref), (weight_hbm, meta_mine.at[: 2 * TAPS]),
        (data_hbm, data_ref), (map_hbm, map_ref),
    )):
        copy = pltpu.make_async_copy(src, dst, arg_sem.at[k])
        copy.start()
        arg_copies.append(copy)
    barrier = pltpu.get_barrier_semaphore()
    peers = [
        (d_bit, d_tile, d_core)
        for d_bit in range(CORES)
        for d_tile in range(tiles)
        for d_core in range(CORES)
        if (d_tile > 0 and d_bit == 0) or (d_tile < 2 and d_tile + d_bit + d_core > 0)
    ]
    for d_bit, d_tile, d_core in peers:
        pl.semaphore_signal(
            barrier,
            inc=1,
            device_id={
                "coil": pair * CORES + (bit + d_bit) % CORES,
                "tile": toggled(tile, d_tile),
                "spk": (core + d_core) % CORES,
            },
            device_id_type=MESH,
        )
    for d in range(CORES, coils):
        pl.semaphore_signal(
            barrier,
            inc=1,
            device_id={
                "coil": (coil + d // CORES * CORES) % coils,
                "spk": (core + d % CORES) % CORES,
            },
            device_id_type=MESH,
        )
    const_copies = []
    for k, (src, dst) in enumerate((
        (perm_hbm, perms), (cell_u_hbm, cell_u), (cell_v_hbm, cell_v), (right_hbm, right),
        (back_hbm, back), (haar_hbm, haar), (fore_hbm, fore),
    )):
        copy = pltpu.make_async_copy(src, dst, const_sem.at[k])
        copy.start()
        const_copies.append(copy)

    mark("prep")
    for copy in arg_copies[:2]:
        copy.wait()
    alive = lax.broadcasted_iota(jnp.int32, (SPK_DEV, n), 0) < count_ref[0]
    bins = bins_ref[...]
    row_of = jnp.where(alive, bins // n, -1).astype(F32)
    col_of = (bins % n).astype(F32)
    meta_mine[2 * TAPS] = row_of.astype(BF16)
    meta_mine[2 * TAPS + 1] = col_of.astype(BF16)
    mark("barrier")
    pl.semaphore_wait(barrier, len(peers) + coils - CORES)

    mark("issue")
    sends = []
    near = [toggled(tile, d) for d in range(tiles)]
    far_first = list(range(tiles // 2, tiles)) + list(range(1, tiles // 2))

    def send(src, dst, s_sem, r_sem, target):
        copy = pltpu.make_async_remote_copy(
            src_ref=src, dst_ref=dst, send_sem=s_sem, recv_sem=r_sem,
            device_id=target, device_id_type=MESH,
        )
        copy.start()
        return copy

    for d in far_first:
        sends.append(send(
            meta_mine, meta_all.at[block], meta_send.at[d], meta_recv.at[block], {"tile": near[d]}
        ))
    sends.append(send(
        meta_mine, meta_all.at[block], meta_send.at[0], meta_recv.at[block], {"spk": 1 - core}
    ))
    inner = []
    across = pair * CORES + 1 - bit
    routes = [{"coil": across, "spk": bit}, {"tile": near[1], "spk": bit},
              {"coil": across, "tile": near[1], "spk": bit}]
    far = [d for d in far_first if d > 1]
    even = [d for d in far if d % 2 == 0]

    def outward(distances):
        return [{"tile": near[d], "spk": bit} for d in distances]

    def spread(src, dst, s_sem, r_sem, targets):
        for k, target in enumerate(targets):
            sends.append(send(src, dst, s_sem.at[1 + k], r_sem, target))
        local_copy = pltpu.make_async_copy(src, dst, r_sem)
        inner_copy = pltpu.make_async_remote_copy(
            src_ref=src, dst_ref=dst, send_sem=s_sem.at[0], recv_sem=r_sem,
            device_id={"spk": 1 - core}, device_id_type=MESH,
        )
        inner.append(inner_copy)

        @pl.when(core == bit)
        def _():
            local_copy.start()

        @pl.when(core != bit)
        def _():
            inner_copy.start()

    arg_copies[2].wait()
    data_wide = data_ref[0].astype(F32)
    data_mine[...] = jnp.concatenate([data_wide[:, 0], data_wide[:, 1]], axis=0).astype(BF16)
    spread(data_mine, data_all.at[block], data_send, data_recv.at[block], routes + outward(far))
    const_copies[0].wait()
    arg_copies[3].wait()
    for p in range(2):
        map_mine[p] = sum(mm_t(x, perms[0]) for x in split(map_ref[0, :, p, :]))
    spread(map_mine, maps.at[:, block], map_send, map_recv.at[block], routes[:1] + outward(even) + routes[1:])

    def arrived(ref, sem):
        pltpu.make_async_copy(ref, ref, sem).wait()

    beyond = [{"coil": across}, {"tile": near[1]}, {"coil": across, "tile": near[1]}]

    def hand_over(ref, s_sem, first, r_sem, targets):
        return (
            pltpu.make_async_copy(ref, ref, r_sem),
            [
                pltpu.make_async_remote_copy(
                    src_ref=ref, dst_ref=ref, send_sem=s_sem.at[first + k], recv_sem=r_sem,
                    device_id=target, device_id_type=MESH,
                )
                for k, target in enumerate(targets)
            ],
        )

    map_hand, data_hand = [], []
    for d in far:
        for c in range(CORES):
            b = near[d] * CORES + c
            data_hand.append(hand_over(
                data_all.at[b], data_send, 2 + tiles + len(data_hand), data_recv.at[b], beyond[:1]
            ))
            if d in even:
                map_hand.append(hand_over(
                    maps.at[:, b], map_send, 2 + tiles + 3 * len(map_hand), map_recv.at[b], beyond
                ))

    def pass_on(hands, where):
        @pl.when((core == bit) & where)
        def _():
            for here, there in hands:
                here.wait()
                for copy in there:
                    copy.start()

    mark("metawait")
    for copy in const_copies[1:]:
        copy.wait()
    meta_all[block] = meta_mine[...]
    for d in range(1, tiles):
        b = near[d] * CORES + core
        arrived(meta_all.at[b], meta_recv.at[b])
        sends.append(send(
            meta_all.at[b], meta_all.at[b], meta_send.at[tiles + d], meta_recv.at[b], {"spk": 1 - core}
        ))
    for d in range(tiles):
        b = near[d] * CORES + 1 - core
        arrived(meta_all.at[b], meta_recv.at[b])

    mark("rank")
    whole = [meta_all[b].reshape(FIELDS * SPK_DEV, n).astype(F32) for b in range(blocks)]

    def field(m):
        return jnp.concatenate([w[m * SPK_DEV : (m + 1) * SPK_DEV] for w in whole], axis=0)

    rows_all = field(2 * TAPS)
    up = lax.broadcasted_iota(jnp.int32, (slots, slots), 0)
    across = lax.broadcasted_iota(jnp.int32, (slots, slots), 1)
    flag = jnp.where(rows_all[:, :LANES] >= 0.0, 1.0 / LANES, 0.0)
    flags = mm_t(jnp.ones((live, LANES), BF16), flag.astype(BF16)).astype(BF16)
    rank = mm(flags, jnp.where(up < across, 1.0, 0.0).astype(BF16))
    here = lax.broadcasted_iota(jnp.int32, (live, slots), 0).astype(F32)
    hit = (flags.astype(F32) > 0.5) & (rank == here)
    pick = jnp.where(hit, 1.0, 0.0).astype(BF16)
    comp = [mm(pick, (rows_all if m == 2 * TAPS else field(m)).astype(BF16)) for m in range(FIELDS)]
    first_low = jnp.broadcast_to(comp[2 * TAPS + 1][:, 1:2], (live, half)) < half

    def halves(x):
        low = jnp.where(first_low, x[:, :half], x[:, half:])
        high = jnp.where(first_low, x[:, half:], x[:, :half])
        return [jnp.concatenate([v[:pair_count], v[pair_count:]], axis=1) for v in (low, high)]

    for m in range(2 * TAPS):
        for o, value in enumerate(halves(comp[m])):
            pairs[o, m] = value
    for m, centre in ((2 * TAPS, comp[2 * TAPS]), (3 * TAPS, comp[2 * TAPS + 1])):
        for t in range(TAPS):
            tap = (centre.astype(jnp.int32) + (t - 1)) & (n - 1)
            for o, value in enumerate(halves(tap.astype(F32))):
                pairs[o, m + t] = value

    mark("pass")
    pass_on(data_hand + map_hand, tile != 0)
    mark("build")

    def build(i, carry):
        def table(cells, m, o):
            def part(k):
                return jnp.broadcast_to(pairs[o, k, pl.ds(i, 1), :].astype(BF16), cells.shape)

            zero = jnp.zeros(cells.shape, BF16)
            return jnp.where(
                cells == part(2 * TAPS + m), part(m),
                jnp.where(
                    cells == part(2 * TAPS + m + 1), part(m + 1),
                    jnp.where(cells == part(2 * TAPS + m + 2), part(m + 2), zero),
                ),
            )

        for o in range(2):
            cells = jnp.concatenate([cell_u[...]] * (n // LANES), axis=1)
            row_tab[i, o] = table(cells, 0, o)
            cells = jnp.concatenate([cell_v[o]] * (n // LANES), axis=1)
            col_tab[i, o] = table(cells, TAPS, o)
        return carry

    lax.fori_loop(0, pair_count // 2, build, 0)

    mark("pass")
    pass_on(data_hand, tile == 0)
    direct = [near[d] * CORES + c for d in range(2) for c in range(CORES)]
    last_maps = [near[d] * CORES + c for d in [0] + list(range(1, tiles, 2)) for c in range(CORES)]

    @pl.when(core == bit)
    def _():
        for b in direct:
            arrived(data_all.at[b], data_recv.at[b])

    mark("build2")
    lax.fori_loop(pair_count // 2, pair_count, build, 0)
    mark("pass")
    pass_on(map_hand, tile == 0)

    mark("datawait")

    @pl.when(core != bit)
    def _():
        for b in range(blocks):
            arrived(data_all.at[b], data_recv.at[b])

    offset = jnp.abs(lax.broadcasted_iota(jnp.int32, (live, n), 1) - half).astype(F32)
    density = (offset + 0.5) * (n / (3.0 * n * live))
    for o, value in enumerate(halves(density)):
        pair_data[o, 2] = value
    every = data_all[...]
    for p in range(2):
        samples = jnp.concatenate(
            [every[b].astype(F32)[p * SPK_DEV : (p + 1) * SPK_DEV] for b in range(blocks)], axis=0
        )
        for o, value in enumerate(halves(mm(pick, samples.astype(BF16)))):
            pair_data[o, p] = value

    first_lane = lax.broadcasted_iota(jnp.int32, (n, half), 1) == 0
    first_row = lax.broadcasted_iota(jnp.int32, (half, half), 0) == 0
    groups = half // MEMBERS
    label = haar_labels(MEMBERS, LEVELS)
    lane = lax.broadcasted_iota(jnp.int32, (1, half), 1) % MEMBERS
    lane_label = jnp.ones((1, half), jnp.int32)
    for level in range(1, LEVELS + 1):
        lane_label = lane_label + jnp.where(lane < MEMBERS >> level, 1, 0)

    def norm_of(k):
        return 1.0 / math.sqrt((haar_signs(MEMBERS, LEVELS)[k] ** 2).sum())

    lane_norm = jnp.zeros((1, half), F32)
    for k in range(MEMBERS):
        lane_norm = jnp.where(lane == k, norm_of(k), lane_norm)
    limits, scales = [], []
    for k in range(MEMBERS):
        band = jnp.minimum(lane_label, int(label[k]))
        limit = jnp.zeros((1, half), F32)
        for level in range(LEVELS):
            limit = jnp.where(band == level + 1, thr_ref[level], limit)
        limits.append(limit)
        scales.append(lane_norm * norm_of(k))
    steps_of = [-STEP_SIZE * scale for scale in scales]
    own_half = block // (blocks // 2)

    copies = []
    for it in range(ITERS):
        slot = it % 2
        mark("spokes")
        grid[...] = jnp.zeros_like(grid)

        def fore_step(step, into, it=it):
            for g in range(GROUP):
                i = step * GROUP + g
                for o in range(2):
                    col = col_tab[i, o].astype(F32)
                    dens = pair_data[o, 2, pl.ds(i, 1), :]
                    seen = mm(kspace[o], row_tab[i, o]) if it > 0 else None
                    for p in range(2):
                        value = -pair_data[o, p, pl.ds(i, 1), :]
                        if it > 0:
                            value = value + jnp.sum(
                                seen[p * window : (p + 1) * window] * col, axis=0, keepdims=True
                            )
                        into[o, p * window : (p + 1) * window, g * n : (g + 1) * n] = (
                            col * (dens * value)
                        ).astype(BF16)

        def back_step(step, source):
            for o in range(2):
                total = None
                for g in range(GROUP):
                    added = mm_t(
                        source[o, :, g * n : (g + 1) * n], row_tab[step * GROUP + g, o]
                    )
                    total = added if total is None else total + added
                grid[o] += total

        turns = pair_count // GROUP // 2
        fore_step(0, smear_a)

        def body(turn, carry):
            back_step(2 * turn, smear_a)
            fore_step(2 * turn + 1, smear_b)
            back_step(2 * turn + 1, smear_b)
            fore_step(2 * turn + 2, smear_a)
            return carry

        lax.fori_loop(0, turns - 1, body, 0)
        back_step(2 * turns - 2, smear_a)
        fore_step(2 * turns - 1, smear_b)
        back_step(2 * turns - 1, smear_b)

        for copy in copies:
            copy.wait_send()

        mark("turned")
        stack = []
        for p in range(2):
            low, high = grid[0, p * window : (p + 1) * window], grid[1, p * window : (p + 1) * window]
            stack += [
                low[:MARGIN] + high[half:], low[MARGIN:half],
                high[:MARGIN] + low[half:], high[MARGIN:half],
            ]
        turned = mm3(split(jnp.concatenate(stack, axis=0)), (right[0], right[1]))
        r_c, i_c = turned[:n, :half], turned[n:, :half]
        r_s, i_s = turned[:n, half:], turned[n:, half:]
        r_z, i_z = jnp.where(first_lane, 0.0, r_s), jnp.where(first_lane, 0.0, i_s)
        sides = [
            split(jnp.concatenate([r_c - i_z, i_c + r_z], axis=1)),
            split(jnp.concatenate(
                [jnp.where(first_lane, r_s, r_c + i_s), jnp.where(first_lane, i_s, i_c - r_s)], axis=1
            )),
        ]
        if it == 0:
            mark("mapwait")

            @pl.when(core != bit)
            def _():
                for b in range(blocks):
                    arrived(maps.at[:, b], map_recv.at[b])

            @pl.when(core == bit)
            def _():
                for b in last_maps:
                    arrived(maps.at[:, b], map_recv.at[b])

            for p in range(2):
                both = sum(
                    lax.dot_general(
                        x, perms[1], (((0,), (1,)), ((), ())), preferred_element_type=F32
                    )
                    for x in split(maps[p].reshape(n, n))
                )
                for q in range(2):
                    sens[p, q] = both[:, q * half : (q + 1) * half]

        mark("image")
        last = it == ITERS - 1
        chunks = [own_half] if last else [0, 1]
        if last:
            sides = [[jnp.where(own_half == 0, a, b) for a, b in zip(*sides)]]
        copies = []
        products = [mm3((back[0], back[1]), side) for side in sides]
        for q, w in zip(chunks, products):
            c_r, c_i, s_r, s_i = w[:half, :half], w[:half, half:], w[half:, :half], w[half:, half:]
            z_r, z_i = jnp.where(first_row, 0.0, s_r), jnp.where(first_row, 0.0, s_i)
            low_r, low_i = c_r - z_i, c_i + z_r
            high_r = jnp.where(first_row, s_r, c_r + s_i)
            high_i = jnp.where(first_row, s_i, c_i - s_r)
            d_r = jnp.concatenate(
                [low_r, pltpu.roll(high_r[:groups], groups - 1, 0), high_r[groups:]], axis=0
            )
            d_i = jnp.concatenate(
                [low_i, pltpu.roll(high_i[:groups], groups - 1, 0), high_i[groups:]], axis=0
            )
            m_r, m_i = sens[0, q], sens[1, q]
            combined = jnp.concatenate([m_r * d_r + m_i * d_i, m_r * d_i - m_i * d_r], axis=1)

            def piece(x, h, m):
                first = h * half + (m if h == 0 else (MEMBERS - m) % MEMBERS) * groups
                return x[first : first + groups]

            along = []
            for h in range(2):
                along += forward_haar([piece(combined, h, m) for m in range(MEMBERS)])
            side = split(jnp.concatenate(along, axis=0))
            grads[slot, q, mine] = mm(side[0], haar[q, 0]) + mm(side[1], haar[q, 0])
            for d in range(1, coils):
                d_pair, d_core = d // CORES, d % CORES
                copy = pltpu.make_async_remote_copy(
                    src_ref=grads.at[slot, q, mine],
                    dst_ref=grads.at[slot, q, mine],
                    send_sem=grad_send.at[slot, q, d],
                    recv_sem=grad_recv.at[slot, q, mine],
                    device_id={
                        "coil": (coil + d_pair * CORES) % coils,
                        "spk": (core + d_core) % CORES,
                    },
                    device_id_type=MESH,
                )
                copy.start()
                copies.append(copy)

        shrunken = []
        for q in chunks:
            mark("gradwait")
            for d in range(1, coils):
                d_pair, d_core = d // CORES, d % CORES
                other = (coil + d_pair * CORES) % coils // CORES * CORES + (core + d_core) % CORES
                pltpu.make_async_copy(
                    grads.at[slot, q, other], grads.at[slot, q, other], grad_recv.at[slot, q, other]
                ).wait()
            mark("shrink")
            summed = grads[slot, q, 0]
            for c in range(1, coils):
                summed = summed + grads[slot, q, c]
            shrunk = []
            for h in range(2):
                for k in range(MEMBERS):
                    at = slice(h * half + k * groups, h * half + (k + 1) * groups)
                    c_r = summed[at, :half] * steps_of[k]
                    c_i = summed[at, half:] * steps_of[k]
                    if it > 0:
                        c_r, c_i = estimate[q, at, :half] + c_r, estimate[q, at, half:] + c_i
                    power = jnp.maximum(c_r * c_r + c_i * c_i, TINY)
                    factor = jnp.maximum(1.0 - limits[k] * lax.rsqrt(power), 0.0)
                    c_r, c_i = c_r * factor, c_i * factor
                    if not last:
                        estimate[q, at, :half], estimate[q, at, half:] = c_r, c_i
                    shrunk.append(jnp.concatenate([c_r * scales[k], c_i * scales[k]], axis=1))
            shrunken.append(split(jnp.concatenate(shrunk, axis=0)))
        fresh_of, seen_of = [], []
        for q, side in zip(chunks, shrunken):
            along = mm(side[0], haar[q, 1]) + mm(side[1], haar[q, 1])
            fresh = []
            for h in range(2):
                first = h * half
                members = inverse_haar(
                    [along[first + k * groups : first + (k + 1) * groups] for k in range(MEMBERS)]
                )
                placed = [None] * MEMBERS
                for m in range(MEMBERS):
                    placed[m if h == 0 else (MEMBERS - m) % MEMBERS] = members[m]
                fresh += placed
            fresh = jnp.concatenate(fresh, axis=0)
            fresh_of.append(fresh)
        if not last:
            mark("fwd")
            for q, fresh in zip(chunks, fresh_of):
                e_r, e_i = fresh[:, :half], fresh[:, half:]
                m_r, m_i = sens[0, q], sens[1, q]
                seen_of.append(split(
                    jnp.concatenate([m_r * e_r - m_i * e_i, m_r * e_i + m_i * e_r], axis=1)
                ))
            for q, w in zip(chunks, [mm3((fore[0], fore[1]), seen) for seen in seen_of]):
                c_r, c_i, s_r, s_i = w[:half, :half], w[:half, half:], w[half:, :half], w[half:, half:]
                z_r, z_i = jnp.where(first_row, 0.0, s_r), jnp.where(first_row, 0.0, s_i)
                v = jnp.concatenate(
                    [
                        c_r + z_i, jnp.where(first_row, s_r, c_r - s_i),
                        c_i - z_r, jnp.where(first_row, s_i, c_i + s_r),
                    ],
                    axis=0,
                )
                half_h[:, q * half : (q + 1) * half], half_l[:, q * half : (q + 1) * half] = split(v)
        if it < ITERS - 1:
            mark("vfft")
            v = mm3((half_h[...], half_l[...]), (right[0], right[1]))
            r_c, i_c, r_s, i_s = v[:n, :half], v[n:, :half], v[:n, half:], v[n:, half:]
            r_z, i_z = jnp.where(first_lane, 0.0, r_s), jnp.where(first_lane, 0.0, i_s)
            whole = [
                jnp.concatenate([r_c + i_z, jnp.where(first_lane, r_s, r_c - i_s)], axis=1).astype(BF16),
                jnp.concatenate([i_c - r_z, jnp.where(first_lane, i_s, i_c + r_s)], axis=1).astype(BF16),
            ]
            for p in range(2):
                first = p * window
                kspace[0, first : first + window] = whole[p][:window]
                kspace[1, first : first + half] = whole[p][half:]
                kspace[1, first + half : first + window] = whole[p][:MARGIN]

    mark("out")
    take = lax.broadcasted_iota(jnp.int32, (rows, half), 0) + block * rows
    at = lax.broadcasted_iota(jnp.int32, (rows, half), 1)
    owner = jnp.where(own_half == 0, at, jnp.where(at == 0, half, n - at))
    chosen = jnp.where(take == owner, 1.0, 0.0).astype(BF16)
    for p in range(2):
        picked = sum(mm_t(chosen, x) for x in split(fresh[:, p * half : (p + 1) * half]))
        result = sum(mm(x, perms[0]) for x in split(picked))
        for t in range(n // LANES):
            out_ref[pl.ds(t * 2 + p, rows, stride=2 * n // LANES), :] = result[:, t * LANES : (t + 1) * LANES]

    @pl.when(core != bit)
    def _():
        for copy in inner:
            copy.wait_send()

    @pl.when(core == bit)
    def _():
        for _, there in data_hand + map_hand:
            for copy in there:
                copy.wait_send()

    for copy in sends + copies:
        copy.wait_send()
    mark(None)


def local(coil_maps, kspace_data, interp_weights, sample_bins, spoke_count, thresholds):
    tiles, coils = lax.axis_size("tile"), lax.axis_size("coil")
    blocks = tiles * CORES
    rows, n = coil_maps.shape[1], coil_maps.shape[3]
    live = blocks * SPK_DEV // 2
    half = n // 2
    window = half + MARGIN
    consts = tables(n)
    vmem = pl.BlockSpec(memory_space=pltpu.VMEM)
    smem = pl.BlockSpec(memory_space=pltpu.SMEM)
    pair_count = live // 2
    dma = pltpu.SemaphoreType.DMA
    any_space = pl.BlockSpec(memory_space=pl.ANY)
    weights = jnp.transpose(interp_weights, (1, 0, 2))
    scratch = [pltpu.VMEM(c.shape, BF16) for c in consts] + [
            pltpu.VMEM(sample_bins.shape, jnp.int32),
            pltpu.VMEM(kspace_data.shape, BF16),
            pltpu.VMEM(coil_maps.shape, F32),
            pltpu.VMEM((FIELDS, SPK_DEV, n), BF16),
            pltpu.VMEM((blocks, FIELDS, SPK_DEV, n), BF16),
            pltpu.VMEM((SPK_DEV * 2, n), BF16),
            pltpu.VMEM((blocks, SPK_DEV * 2, n), BF16),
            pltpu.VMEM((2, rows, n), F32),
            pltpu.VMEM((2, blocks, rows, n), F32),
            pltpu.VMEM((2, 4 * TAPS, pair_count, n), F32),
            pltpu.VMEM((2, 3, pair_count, n), F32),
            pltpu.VMEM((pair_count, 2, n, n), BF16),
            pltpu.VMEM((pair_count, 2, window, n), BF16),
            pltpu.VMEM((2, 2 * window, n), BF16),
            pltpu.VMEM((2, 2 * window, n), F32),
            pltpu.VMEM((2, 2 * window, GROUP * n), BF16),
            pltpu.VMEM((2, 2 * window, GROUP * n), BF16),
            pltpu.VMEM((2 * n, n), BF16),
            pltpu.VMEM((2 * n, n), BF16),
            pltpu.VMEM((2, n, n), F32),
            pltpu.VMEM((2, 2, coils, n, n), F32),
            pltpu.VMEM((2, 2, n, half), F32),
    ]
    out = pl.pallas_call(
        functools.partial(kernel, (n, tiles, coils, rows, live)),
        out_shape=jax.ShapeDtypeStruct((rows * 2 * n // LANES, LANES), F32),
        in_specs=[smem, smem] + [any_space] * (4 + len(consts)),
        out_specs=vmem,
        scratch_shapes=scratch + [
            dma((len(consts),)), dma((4,)),
            dma((blocks,)), dma((blocks,)), dma((2 + tiles + 3 * blocks,)), dma((blocks,)),
            dma((2 + tiles + 3 * blocks,)), dma((blocks,)),
            dma((2, 2, coils)), dma((2, 2, coils)),
        ],
        compiler_params=pltpu.CompilerParams(
            has_side_effects=True, collective_id=0, vmem_limit_bytes=VMEM_LIMIT
        ),
    )(thresholds, spoke_count, weights, sample_bins, kspace_data, coil_maps, *consts)
    out = out.reshape(rows, n // LANES, 2, LANES)
    return jnp.transpose(out, (0, 2, 1, 3)).reshape(rows, 2, n)


def solution(mesh):
    placed = (
        P("coil", ("grp", "tile", "spk"), None, None),
        P("coil", ("grp", "tile", "spk"), None, None),
        P(("grp", "tile", "spk"), None, None),
        P(("grp", "tile", "spk"), None),
        P(("grp", "tile", "spk")),
        P(),
    )
    return jax.shard_map(
        local,
        mesh=mesh,
        in_specs=placed,
        out_specs=P(("grp", "tile", "spk"), None, None),
        check_vma=False,
    )
```

```python
import functools
import math

import jax
import jax.numpy as jnp
import numpy as np
from jax import lax
from jax.experimental import pallas as pl
from jax.experimental.pallas import tpu as pltpu
from jax.sharding import PartitionSpec as P

SPK_DEV = 8
LEVELS = 3
MEMBERS = 2**LEVELS
ITERS = 4
CORES = 2
GROUP = 4
TAPS = 3
FIELDS = 8
MARGIN = 16
STEP_SIZE = 0.5
LANES = 128
TINY = 1e-30
VMEM_LIMIT = 60 * 1024 * 1024
F32 = jnp.float32
BF16 = jnp.bfloat16
MESH = pl.DeviceIdType.MESH

_scope = [None]


def mark(name):
    if _scope[0] is not None:
        _scope[0].__exit__(None, None, None)
        _scope[0] = None
    if name:
        _scope[0] = jax.named_scope(name)
        _scope[0].__enter__()


def split_np(table):
    table = np.ascontiguousarray(table).astype(np.float32)
    high = table.astype(jnp.bfloat16)
    low = (table - high.astype(np.float32)).astype(jnp.bfloat16)
    return high, low


def haar_signs(length, levels):
    mat = np.eye(length)
    for level in range(levels):
        span = length >> level
        half = span // 2
        step = np.eye(length)
        step[:span] = 0.0
        for i in range(half):
            step[i, 2 * i] = step[i, 2 * i + 1] = 1.0
            step[half + i, 2 * i] = 1.0
            step[half + i, 2 * i + 1] = -1.0
        mat = step @ mat
    return mat


def haar_labels(length, levels):
    label = np.ones((length,), np.int32)
    for level in range(1, levels + 1):
        label = label + (np.arange(length) < length >> level)
    return label


def mirror(first, n):
    second = (n - first) % n
    second[first == 0] = n // 2
    return np.concatenate([first, second])


def orders(n):
    half = n // 2
    by_lane = mirror(np.arange(half), n)
    edge = MARGIN // 2
    near = np.concatenate([np.arange(edge), np.arange(half - edge, half), np.arange(edge, half - edge)])
    by_freq = mirror(near, n)
    groups = half // MEMBERS
    member = np.arange(half) // groups
    group = np.arange(half) % groups
    low = MEMBERS * group + member
    high = n - MEMBERS * group - member
    high[:groups] = n - MEMBERS * (np.arange(groups) + 1)
    by_pixel = np.concatenate([low, high])
    return by_lane, by_freq, low, by_pixel


def tables(n):
    half = n // 2
    by_lane, by_freq, low, by_pixel = orders(n)
    phase = np.outer(np.arange(n), np.arange(n)) % n
    angle = phase * (2.0 * np.pi / n)
    cosine = np.cos(angle) / math.sqrt(n)
    sine = np.sin(angle) / math.sqrt(n)

    def folded(outs, ins):
        bottom = sine[outs][:, ins]
        bottom[outs == 0] = cosine[half][ins]
        return np.concatenate([cosine[outs][:, ins], bottom], axis=0)

    right = folded(np.arange(half), by_lane).T
    back = folded(low, by_freq)
    fore = folded(by_freq[:half], by_pixel)
    small = haar_signs(MEMBERS, LEVELS)
    chunk_haar = []
    for q in range(2):
        pixels = by_lane[q * half : (q + 1) * half]
        mat = np.zeros((half, half))
        group = pixels // MEMBERS - q * (half // MEMBERS)
        for k in range(MEMBERS):
            mat[group * MEMBERS + k, np.arange(half)] = small[k, pixels % MEMBERS]
        both = np.kron(np.eye(2), mat)
        chunk_haar.append((both.T, both))
    haar = np.stack([np.stack(pair) for pair in chunk_haar]).astype(jnp.bfloat16)
    windows = np.stack(
        [by_freq[: half + MARGIN], np.concatenate([by_freq[half:], by_freq[:MARGIN]])]
    )
    cell_u = np.repeat(by_lane[:, None], LANES, axis=1).astype(jnp.bfloat16)
    cell_v = np.repeat(windows[:, :, None], LANES, axis=2).astype(jnp.bfloat16)
    turn_s = np.zeros((n, n))
    turn_s[np.arange(n), by_pixel] = 1.0
    turn_r = np.zeros((n, n))
    turn_r[np.arange(n), by_lane] = 1.0
    perms = np.stack([turn_s, turn_r]).astype(jnp.bfloat16)
    return (
        np.stack(split_np(right)), np.stack(split_np(back)), np.stack(split_np(fore)),
        haar, cell_u, cell_v, perms,
    )


def split(x):
    high = x.astype(BF16)
    return high, (x - high.astype(F32)).astype(BF16)


def mm(a, b):
    return jnp.dot(a, b, preferred_element_type=F32)


def mm_t(a, b):
    return lax.dot_general(a, b, (((1,), (1,)), ((), ())), preferred_element_type=F32)


def mm3(a, b):
    return mm(a[0], b[0]) + (mm(a[0], b[1]) + mm(a[1], b[0]))


def forward_haar(x):
    sums = [x[2 * i] + x[2 * i + 1] for i in range(4)]
    out = [None] * 4 + [x[2 * i] - x[2 * i + 1] for i in range(4)]
    pair = [sums[0] + sums[1], sums[2] + sums[3]]
    out[2], out[3] = sums[0] - sums[1], sums[2] - sums[3]
    out[0], out[1] = pair[0] + pair[1], pair[0] - pair[1]
    return out


def inverse_haar(c):
    pair = [c[0] + c[1], c[0] - c[1]]
    sums = [pair[0] + c[2], pair[0] - c[2], pair[1] + c[3], pair[1] - c[3]]
    out = []
    for i in range(4):
        out += [sums[i] + c[4 + i], sums[i] - c[4 + i]]
    return out


def kernel(
    dims,
    thr_ref, count_ref, weight_hbm, bins_hbm, data_hbm, map_hbm,
    right_hbm, back_hbm, fore_hbm, haar_hbm, cell_u_hbm, cell_v_hbm, perm_hbm,
    out_ref,
    right, back, fore, haar, cell_u, cell_v, perms,
    bins_ref, data_ref, map_ref, meta_mine, meta_all, data_mine, data_all, map_mine, maps,
    pairs, pair_data, row_tab, col_tab, kspace, grid, smear_a, smear_b,
    half_h, half_l, estimate, grads, sens,
    const_sem, arg_sem, meta_send, meta_recv, data_send, data_recv, map_send, map_recv, grad_send, grad_recv,
):
    n, tiles, coils, rows, live = dims
    half = n // 2
    window = half + MARGIN
    blocks = tiles * CORES
    slots = blocks * SPK_DEV
    pair_count = live // 2
    coil, tile, core = lax.axis_index("coil"), lax.axis_index("tile"), lax.axis_index("spk")
    pair, bit = coil // CORES, coil % CORES
    block = tile * CORES + core
    mine = pair * CORES + core

    def toggled(value, d):
        step = 1
        while step <= d:
            if d & step:
                value = value + step - 2 * step * (value // step % 2)
            step *= 2
        return value

    mark("start")
    arg_copies = []
    for k, (src, dst) in enumerate((
        (bins_hbm, bins_ref), (weight_hbm, meta_mine.at[: 2 * TAPS]),
        (data_hbm, data_ref), (map_hbm, map_ref),
    )):
        copy = pltpu.make_async_copy(src, dst, arg_sem.at[k])
        copy.start()
        arg_copies.append(copy)
    barrier = pltpu.get_barrier_semaphore()
    peers = [
        (d_bit, d_tile, d_core)
        for d_bit in range(CORES)
        for d_tile in range(tiles)
        for d_core in range(CORES)
        if (d_tile > 0 and d_bit == 0) or (d_tile < 2 and d_tile + d_bit + d_core > 0)
    ]
    for d_bit, d_tile, d_core in peers:
        pl.semaphore_signal(
            barrier,
            inc=1,
            device_id={
                "coil": pair * CORES + (bit + d_bit) % CORES,
                "tile": toggled(tile, d_tile),
                "spk": (core + d_core) % CORES,
            },
            device_id_type=MESH,
        )
    for d in range(CORES, coils):
        pl.semaphore_signal(
            barrier,
            inc=1,
            device_id={
                "coil": (coil + d // CORES * CORES) % coils,
                "spk": (core + d % CORES) % CORES,
            },
            device_id_type=MESH,
        )
    const_copies = []
    for k, (src, dst) in enumerate((
        (perm_hbm, perms), (cell_u_hbm, cell_u), (cell_v_hbm, cell_v), (right_hbm, right),
        (back_hbm, back), (haar_hbm, haar), (fore_hbm, fore),
    )):
        copy = pltpu.make_async_copy(src, dst, const_sem.at[k])
        copy.start()
        const_copies.append(copy)

    mark("prep")
    for copy in arg_copies[:2]:
        copy.wait()
    alive = lax.broadcasted_iota(jnp.int32, (SPK_DEV, n), 0) < count_ref[0]
    bins = bins_ref[...]
    row_of = jnp.where(alive, bins // n, -1).astype(F32)
    col_of = (bins % n).astype(F32)
    meta_mine[2 * TAPS] = row_of.astype(BF16)
    meta_mine[2 * TAPS + 1] = col_of.astype(BF16)
    mark("barrier")
    pl.semaphore_wait(barrier, len(peers) + coils - CORES)

    mark("issue")
    sends = []
    near = [toggled(tile, d) for d in range(tiles)]
    far_first = list(range(tiles // 2, tiles)) + list(range(1, tiles // 2))

    def send(src, dst, s_sem, r_sem, target):
        copy = pltpu.make_async_remote_copy(
            src_ref=src, dst_ref=dst, send_sem=s_sem, recv_sem=r_sem,
            device_id=target, device_id_type=MESH,
        )
        copy.start()
        return copy

    for d in far_first:
        sends.append(send(
            meta_mine, meta_all.at[block], meta_send.at[d], meta_recv.at[block], {"tile": near[d]}
        ))
    sends.append(send(
        meta_mine, meta_all.at[block], meta_send.at[0], meta_recv.at[block], {"spk": 1 - core}
    ))
    inner = []
    across = pair * CORES + 1 - bit
    routes = [{"coil": across, "spk": bit}, {"tile": near[1], "spk": bit},
              {"coil": across, "tile": near[1], "spk": bit}]
    far = [d for d in far_first if d > 1]
    even = [d for d in far if d % 2 == 0]

    def outward(distances):
        return [{"tile": near[d], "spk": bit} for d in distances]

    def spread(src, dst, s_sem, r_sem, targets):
        for k, target in enumerate(targets):
            sends.append(send(src, dst, s_sem.at[1 + k], r_sem, target))
        local_copy = pltpu.make_async_copy(src, dst, r_sem)
        inner_copy = pltpu.make_async_remote_copy(
            src_ref=src, dst_ref=dst, send_sem=s_sem.at[0], recv_sem=r_sem,
            device_id={"spk": 1 - core}, device_id_type=MESH,
        )
        inner.append(inner_copy)

        @pl.when(core == bit)
        def _():
            local_copy.start()

        @pl.when(core != bit)
        def _():
            inner_copy.start()

    arg_copies[2].wait()
    data_wide = data_ref[0].astype(F32)
    data_mine[...] = jnp.concatenate([data_wide[:, 0], data_wide[:, 1]], axis=0).astype(BF16)
    spread(data_mine, data_all.at[block], data_send, data_recv.at[block], routes + outward(far))
    const_copies[0].wait()
    arg_copies[3].wait()
    for p in range(2):
        map_mine[p] = sum(mm_t(x, perms[0]) for x in split(map_ref[0, :, p, :]))
    spread(map_mine, maps.at[:, block], map_send, map_recv.at[block], outward(even) + routes[::-1])

    def arrived(ref, sem):
        pltpu.make_async_copy(ref, ref, sem).wait()

    beyond = [{"coil": across}, {"tile": near[1]}, {"coil": across, "tile": near[1]}]

    def hand_over(ref, s_sem, first, r_sem, targets):
        return (
            pltpu.make_async_copy(ref, ref, r_sem),
            [
                pltpu.make_async_remote_copy(
                    src_ref=ref, dst_ref=ref, send_sem=s_sem.at[first + k], recv_sem=r_sem,
                    device_id=target, device_id_type=MESH,
                )
                for k, target in enumerate(targets)
            ],
        )

    map_hand, data_hand = [], []
    for d in far:
        for c in range(CORES):
            b = near[d] * CORES + c
            data_hand.append(hand_over(
                data_all.at[b], data_send, 2 + tiles + len(data_hand), data_recv.at[b], beyond[:1]
            ))
            if d in even:
                map_hand.append(hand_over(
                    maps.at[:, b], map_send, 2 + tiles + 3 * len(map_hand), map_recv.at[b], beyond
                ))

    def pass_on(hands, where):
        @pl.when((core == bit) & where)
        def _():
            for here, there in hands:
                here.wait()
                for copy in there:
                    copy.start()

    mark("metawait")
    for copy in const_copies[1:]:
        copy.wait()
    meta_all[block] = meta_mine[...]
    for d in range(1, tiles):
        b = near[d] * CORES + core
        arrived(meta_all.at[b], meta_recv.at[b])
        sends.append(send(
            meta_all.at[b], meta_all.at[b], meta_send.at[tiles + d], meta_recv.at[b], {"spk": 1 - core}
        ))
    for d in range(tiles):
        b = near[d] * CORES + 1 - core
        arrived(meta_all.at[b], meta_recv.at[b])

    mark("rank")
    whole = [meta_all[b].reshape(FIELDS * SPK_DEV, n).astype(F32) for b in range(blocks)]

    def field(m):
        return jnp.concatenate([w[m * SPK_DEV : (m + 1) * SPK_DEV] for w in whole], axis=0)

    rows_all = field(2 * TAPS)
    up = lax.broadcasted_iota(jnp.int32, (slots, slots), 0)
    across = lax.broadcasted_iota(jnp.int32, (slots, slots), 1)
    flag = jnp.where(rows_all[:, :LANES] >= 0.0, 1.0 / LANES, 0.0)
    flags = mm_t(jnp.ones((live, LANES), BF16), flag.astype(BF16)).astype(BF16)
    rank = mm(flags, jnp.where(up < across, 1.0, 0.0).astype(BF16))
    here = lax.broadcasted_iota(jnp.int32, (live, slots), 0).astype(F32)
    hit = (flags.astype(F32) > 0.5) & (rank == here)
    pick = jnp.where(hit, 1.0, 0.0).astype(BF16)
    comp = [mm(pick, (rows_all if m == 2 * TAPS else field(m)).astype(BF16)) for m in range(FIELDS)]
    first_low = jnp.broadcast_to(comp[2 * TAPS + 1][:, 1:2], (live, half)) < half

    def halves(x):
        low = jnp.where(first_low, x[:, :half], x[:, half:])
        high = jnp.where(first_low, x[:, half:], x[:, :half])
        return [jnp.concatenate([v[:pair_count], v[pair_count:]], axis=1) for v in (low, high)]

    for m in range(2 * TAPS):
        for o, value in enumerate(halves(comp[m])):
            pairs[o, m] = value
    for m, centre in ((2 * TAPS, comp[2 * TAPS]), (3 * TAPS, comp[2 * TAPS + 1])):
        for t in range(TAPS):
            tap = (centre.astype(jnp.int32) + (t - 1)) & (n - 1)
            for o, value in enumerate(halves(tap.astype(F32))):
                pairs[o, m + t] = value

    mark("pass")
    pass_on(data_hand + map_hand, tile != 0)
    mark("build")

    def build(i, carry):
        def table(cells, m, o):
            def part(k):
                return jnp.broadcast_to(pairs[o, k, pl.ds(i, 1), :].astype(BF16), cells.shape)

            zero = jnp.zeros(cells.shape, BF16)
            return jnp.where(
                cells == part(2 * TAPS + m), part(m),
                jnp.where(
                    cells == part(2 * TAPS + m + 1), part(m + 1),
                    jnp.where(cells == part(2 * TAPS + m + 2), part(m + 2), zero),
                ),
            )

        for o in range(2):
            cells = jnp.concatenate([cell_u[...]] * (n // LANES), axis=1)
            row_tab[i, o] = table(cells, 0, o)
            cells = jnp.concatenate([cell_v[o]] * (n // LANES), axis=1)
            col_tab[i, o] = table(cells, TAPS, o)
        return carry

    lax.fori_loop(0, pair_count // 2, build, 0)

    mark("pass")
    pass_on(data_hand, tile == 0)
    direct = [near[d] * CORES + c for d in range(2) for c in range(CORES)]
    last_maps = [near[d] * CORES + c for d in [0] + list(range(1, tiles, 2)) for c in range(CORES)]

    @pl.when(core == bit)
    def _():
        for b in direct:
            arrived(data_all.at[b], data_recv.at[b])

    mark("build2")
    lax.fori_loop(pair_count // 2, pair_count, build, 0)
    mark("pass")
    pass_on(map_hand, tile == 0)

    mark("datawait")

    @pl.when(core != bit)
    def _():
        for b in range(blocks):
            arrived(data_all.at[b], data_recv.at[b])

    offset = jnp.abs(lax.broadcasted_iota(jnp.int32, (live, n), 1) - half).astype(F32)
    density = (offset + 0.5) * (n / (3.0 * n * live))
    for o, value in enumerate(halves(density)):
        pair_data[o, 2] = value
    every = data_all[...]
    for p in range(2):
        samples = jnp.concatenate(
            [every[b].astype(F32)[p * SPK_DEV : (p + 1) * SPK_DEV] for b in range(blocks)], axis=0
        )
        for o, value in enumerate(halves(mm(pick, samples.astype(BF16)))):
            pair_data[o, p] = value

    first_lane = lax.broadcasted_iota(jnp.int32, (n, half), 1) == 0
    first_row = lax.broadcasted_iota(jnp.int32, (half, half), 0) == 0
    groups = half // MEMBERS
    label = haar_labels(MEMBERS, LEVELS)
    lane = lax.broadcasted_iota(jnp.int32, (1, half), 1) % MEMBERS
    lane_label = jnp.ones((1, half), jnp.int32)
    for level in range(1, LEVELS + 1):
        lane_label = lane_label + jnp.where(lane < MEMBERS >> level, 1, 0)

    def norm_of(k):
        return 1.0 / math.sqrt((haar_signs(MEMBERS, LEVELS)[k] ** 2).sum())

    lane_norm = jnp.zeros((1, half), F32)
    for k in range(MEMBERS):
        lane_norm = jnp.where(lane == k, norm_of(k), lane_norm)
    limits, scales = [], []
    for k in range(MEMBERS):
        band = jnp.minimum(lane_label, int(label[k]))
        limit = jnp.zeros((1, half), F32)
        for level in range(LEVELS):
            limit = jnp.where(band == level + 1, thr_ref[level], limit)
        limits.append(limit)
        scales.append(lane_norm * norm_of(k))
    steps_of = [-STEP_SIZE * scale for scale in scales]
    own_half = block // (blocks // 2)

    copies = []
    for it in range(ITERS):
        slot = it % 2
        mark("spokes")

        def fore_step(step, into, it=it):
            for g in range(GROUP):
                i = step * GROUP + g
                for o in range(2):
                    col = col_tab[i, o].astype(F32)
                    dens = pair_data[o, 2, pl.ds(i, 1), :]
                    seen = mm(kspace[o], row_tab[i, o]) if it > 0 else None
                    for p in range(2):
                        value = -pair_data[o, p, pl.ds(i, 1), :]
                        if it > 0:
                            value = value + jnp.sum(
                                seen[p * window : (p + 1) * window] * col, axis=0, keepdims=True
                            )
                        into[o, p * window : (p + 1) * window, g * n : (g + 1) * n] = (
                            col * (dens * value)
                        ).astype(BF16)

        def back_step(step, source, opens=False):
            for o in range(2):
                total = None
                for g in range(GROUP):
                    added = mm_t(
                        source[o, :, g * n : (g + 1) * n], row_tab[step * GROUP + g, o]
                    )
                    total = added if total is None else total + added
                grid[o] = total if opens else grid[o] + total

        turns = pair_count // GROUP // 2
        fore_step(0, smear_a)

        def body(turn, carry, opens=False):
            back_step(2 * turn, smear_a, opens)
            fore_step(2 * turn + 1, smear_b)
            back_step(2 * turn + 1, smear_b)
            fore_step(2 * turn + 2, smear_a)
            return carry

        if turns > 1:
            body(0, 0, True)
            if turns > 2:
                lax.fori_loop(1, turns - 1, body, 0)
        back_step(2 * turns - 2, smear_a, turns == 1)
        fore_step(2 * turns - 1, smear_b)
        back_step(2 * turns - 1, smear_b)

        for copy in copies:
            copy.wait_send()

        mark("turned")
        stack = []
        for p in range(2):
            low, high = grid[0, p * window : (p + 1) * window], grid[1, p * window : (p + 1) * window]
            stack += [
                low[:MARGIN] + high[half:], low[MARGIN:half],
                high[:MARGIN] + low[half:], high[MARGIN:half],
            ]
        turned = mm3(split(jnp.concatenate(stack, axis=0)), (right[0], right[1]))
        r_c, i_c = turned[:n, :half], turned[n:, :half]
        r_s, i_s = turned[:n, half:], turned[n:, half:]
        r_z, i_z = jnp.where(first_lane, 0.0, r_s), jnp.where(first_lane, 0.0, i_s)
        sides = [
            split(jnp.concatenate([r_c - i_z, i_c + r_z], axis=1)),
            split(jnp.concatenate(
                [jnp.where(first_lane, r_s, r_c + i_s), jnp.where(first_lane, i_s, i_c - r_s)], axis=1
            )),
        ]
        if it == 0:
            mark("mapwait")

            @pl.when(core != bit)
            def _():
                for b in range(blocks):
                    arrived(maps.at[:, b], map_recv.at[b])

            @pl.when(core == bit)
            def _():
                for b in last_maps:
                    arrived(maps.at[:, b], map_recv.at[b])

            for p in range(2):
                both = sum(
                    lax.dot_general(
                        x, perms[1], (((0,), (1,)), ((), ())), preferred_element_type=F32
                    )
                    for x in split(maps[p].reshape(n, n))
                )
                for q in range(2):
                    sens[p, q] = both[:, q * half : (q + 1) * half]

        mark("image")
        last = it == ITERS - 1
        chunks = [own_half] if last else [0, 1]
        if last:
            sides = [[jnp.where(own_half == 0, a, b) for a, b in zip(*sides)]]
        copies = []
        products = [mm3((back[0], back[1]), side) for side in sides]
        for q, w in zip(chunks, products):
            c_r, c_i, s_r, s_i = w[:half, :half], w[:half, half:], w[half:, :half], w[half:, half:]
            z_r, z_i = jnp.where(first_row, 0.0, s_r), jnp.where(first_row, 0.0, s_i)
            low_r, low_i = c_r - z_i, c_i + z_r
            high_r = jnp.where(first_row, s_r, c_r + s_i)
            high_i = jnp.where(first_row, s_i, c_i - s_r)
            d_r = jnp.concatenate(
                [low_r, pltpu.roll(high_r[:groups], groups - 1, 0), high_r[groups:]], axis=0
            )
            d_i = jnp.concatenate(
                [low_i, pltpu.roll(high_i[:groups], groups - 1, 0), high_i[groups:]], axis=0
            )
            m_r, m_i = sens[0, q], sens[1, q]
            combined = jnp.concatenate([m_r * d_r + m_i * d_i, m_r * d_i - m_i * d_r], axis=1)

            def piece(x, h, m):
                first = h * half + (m if h == 0 else (MEMBERS - m) % MEMBERS) * groups
                return x[first : first + groups]

            along = []
            for h in range(2):
                along += forward_haar([piece(combined, h, m) for m in range(MEMBERS)])
            side = split(jnp.concatenate(along, axis=0))
            grads[slot, q, mine] = mm(side[0], haar[q, 0]) + mm(side[1], haar[q, 0])
            for d in range(1, coils):
                d_pair, d_core = d // CORES, d % CORES
                copy = pltpu.make_async_remote_copy(
                    src_ref=grads.at[slot, q, mine],
                    dst_ref=grads.at[slot, q, mine],
                    send_sem=grad_send.at[slot, q, d],
                    recv_sem=grad_recv.at[slot, q, mine],
                    device_id={
                        "coil": (coil + d_pair * CORES) % coils,
                        "spk": (core + d_core) % CORES,
                    },
                    device_id_type=MESH,
                )
                copy.start()
                copies.append(copy)

        shrunken = []
        for q in chunks:
            mark("gradwait")
            for d in range(1, coils):
                d_pair, d_core = d // CORES, d % CORES
                other = (coil + d_pair * CORES) % coils // CORES * CORES + (core + d_core) % CORES
                pltpu.make_async_copy(
                    grads.at[slot, q, other], grads.at[slot, q, other], grad_recv.at[slot, q, other]
                ).wait()
            mark("shrink")
            summed = grads[slot, q, 0]
            for c in range(1, coils):
                summed = summed + grads[slot, q, c]
            shrunk = []
            for h in range(2):
                for k in range(MEMBERS):
                    at = slice(h * half + k * groups, h * half + (k + 1) * groups)
                    c_r = summed[at, :half] * steps_of[k]
                    c_i = summed[at, half:] * steps_of[k]
                    if it > 0:
                        c_r, c_i = estimate[q, at, :half] + c_r, estimate[q, at, half:] + c_i
                    power = jnp.maximum(c_r * c_r + c_i * c_i, TINY)
                    factor = jnp.maximum(1.0 - limits[k] * lax.rsqrt(power), 0.0)
                    c_r, c_i = c_r * factor, c_i * factor
                    if not last:
                        estimate[q, at, :half], estimate[q, at, half:] = c_r, c_i
                    shrunk.append(jnp.concatenate([c_r * scales[k], c_i * scales[k]], axis=1))
            shrunken.append(split(jnp.concatenate(shrunk, axis=0)))
        fresh_of, seen_of = [], []
        for q, side in zip(chunks, shrunken):
            along = mm(side[0], haar[q, 1]) + mm(side[1], haar[q, 1])
            fresh = []
            for h in range(2):
                first = h * half
                members = inverse_haar(
                    [along[first + k * groups : first + (k + 1) * groups] for k in range(MEMBERS)]
                )
                placed = [None] * MEMBERS
                for m in range(MEMBERS):
                    placed[m if h == 0 else (MEMBERS - m) % MEMBERS] = members[m]
                fresh += placed
            fresh = jnp.concatenate(fresh, axis=0)
            fresh_of.append(fresh)
        if not last:
            mark("fwd")
            for q, fresh in zip(chunks, fresh_of):
                e_r, e_i = fresh[:, :half], fresh[:, half:]
                m_r, m_i = sens[0, q], sens[1, q]
                seen_of.append(split(
                    jnp.concatenate([m_r * e_r - m_i * e_i, m_r * e_i + m_i * e_r], axis=1)
                ))
            for q, w in zip(chunks, [mm3((fore[0], fore[1]), seen) for seen in seen_of]):
                c_r, c_i, s_r, s_i = w[:half, :half], w[:half, half:], w[half:, :half], w[half:, half:]
                z_r, z_i = jnp.where(first_row, 0.0, s_r), jnp.where(first_row, 0.0, s_i)
                v = jnp.concatenate(
                    [
                        c_r + z_i, jnp.where(first_row, s_r, c_r - s_i),
                        c_i - z_r, jnp.where(first_row, s_i, c_i + s_r),
                    ],
                    axis=0,
                )
                half_h[:, q * half : (q + 1) * half], half_l[:, q * half : (q + 1) * half] = split(v)
        if it < ITERS - 1:
            mark("vfft")
            v = mm3((half_h[...], half_l[...]), (right[0], right[1]))
            r_c, i_c, r_s, i_s = v[:n, :half], v[n:, :half], v[:n, half:], v[n:, half:]
            r_z, i_z = jnp.where(first_lane, 0.0, r_s), jnp.where(first_lane, 0.0, i_s)
            whole = [
                jnp.concatenate([r_c + i_z, jnp.where(first_lane, r_s, r_c - i_s)], axis=1).astype(BF16),
                jnp.concatenate([i_c - r_z, jnp.where(first_lane, i_s, i_c + r_s)], axis=1).astype(BF16),
            ]
            for p in range(2):
                first = p * window
                kspace[0, first : first + window] = whole[p][:window]
                kspace[1, first : first + half] = whole[p][half:]
                kspace[1, first + half : first + window] = whole[p][:MARGIN]

    mark("out")
    take = lax.broadcasted_iota(jnp.int32, (rows, half), 0) + block * rows
    at = lax.broadcasted_iota(jnp.int32, (rows, half), 1)
    owner = jnp.where(own_half == 0, at, jnp.where(at == 0, half, n - at))
    chosen = jnp.where(take == owner, 1.0, 0.0).astype(BF16)
    for p in range(2):
        picked = sum(mm_t(chosen, x) for x in split(fresh[:, p * half : (p + 1) * half]))
        result = sum(mm(x, perms[0]) for x in split(picked))
        for t in range(n // LANES):
            out_ref[pl.ds(t * 2 + p, rows, stride=2 * n // LANES), :] = result[:, t * LANES : (t + 1) * LANES]

    @pl.when(core != bit)
    def _():
        for copy in inner:
            copy.wait_send()

    @pl.when(core == bit)
    def _():
        for _, there in data_hand + map_hand:
            for copy in there:
                copy.wait_send()

    for copy in sends + copies:
        copy.wait_send()
    mark(None)


def local(coil_maps, kspace_data, interp_weights, sample_bins, spoke_count, thresholds):
    tiles, coils = lax.axis_size("tile"), lax.axis_size("coil")
    blocks = tiles * CORES
    rows, n = coil_maps.shape[1], coil_maps.shape[3]
    live = blocks * SPK_DEV // 2
    half = n // 2
    window = half + MARGIN
    consts = tables(n)
    vmem = pl.BlockSpec(memory_space=pltpu.VMEM)
    smem = pl.BlockSpec(memory_space=pltpu.SMEM)
    pair_count = live // 2
    dma = pltpu.SemaphoreType.DMA
    any_space = pl.BlockSpec(memory_space=pl.ANY)
    weights = jnp.transpose(interp_weights, (1, 0, 2))
    scratch = [pltpu.VMEM(c.shape, BF16) for c in consts] + [
            pltpu.VMEM(sample_bins.shape, jnp.int32),
            pltpu.VMEM(kspace_data.shape, BF16),
            pltpu.VMEM(coil_maps.shape, F32),
            pltpu.VMEM((FIELDS, SPK_DEV, n), BF16),
            pltpu.VMEM((blocks, FIELDS, SPK_DEV, n), BF16),
            pltpu.VMEM((SPK_DEV * 2, n), BF16),
            pltpu.VMEM((blocks, SPK_DEV * 2, n), BF16),
            pltpu.VMEM((2, rows, n), F32),
            pltpu.VMEM((2, blocks, rows, n), F32),
            pltpu.VMEM((2, 4 * TAPS, pair_count, n), F32),
            pltpu.VMEM((2, 3, pair_count, n), F32),
            pltpu.VMEM((pair_count, 2, n, n), BF16),
            pltpu.VMEM((pair_count, 2, window, n), BF16),
            pltpu.VMEM((2, 2 * window, n), BF16),
            pltpu.VMEM((2, 2 * window, n), F32),
            pltpu.VMEM((2, 2 * window, GROUP * n), BF16),
            pltpu.VMEM((2, 2 * window, GROUP * n), BF16),
            pltpu.VMEM((2 * n, n), BF16),
            pltpu.VMEM((2 * n, n), BF16),
            pltpu.VMEM((2, n, n), F32),
            pltpu.VMEM((2, 2, coils, n, n), F32),
            pltpu.VMEM((2, 2, n, half), F32),
    ]
    out = pl.pallas_call(
        functools.partial(kernel, (n, tiles, coils, rows, live)),
        out_shape=jax.ShapeDtypeStruct((rows * 2 * n // LANES, LANES), F32),
        in_specs=[smem, smem] + [any_space] * (4 + len(consts)),
        out_specs=vmem,
        scratch_shapes=scratch + [
            dma((len(consts),)), dma((4,)),
            dma((blocks,)), dma((blocks,)), dma((2 + tiles + 3 * blocks,)), dma((blocks,)),
            dma((2 + tiles + 3 * blocks,)), dma((blocks,)),
            dma((2, 2, coils)), dma((2, 2, coils)),
        ],
        compiler_params=pltpu.CompilerParams(
            has_side_effects=True, collective_id=0, vmem_limit_bytes=VMEM_LIMIT
        ),
    )(thresholds, spoke_count, weights, sample_bins, kspace_data, coil_maps, *consts)
    out = out.reshape(rows, n // LANES, 2, LANES)
    return jnp.transpose(out, (0, 2, 1, 3)).reshape(rows, 2, n)


def solution(mesh):
    placed = (
        P("coil", ("grp", "tile", "spk"), None, None),
        P("coil", ("grp", "tile", "spk"), None, None),
        P(("grp", "tile", "spk"), None, None),
        P(("grp", "tile", "spk"), None),
        P(("grp", "tile", "spk")),
        P(),
    )
    return jax.shard_map(
        local,
        mesh=mesh,
        in_specs=placed,
        out_specs=P(("grp", "tile", "spk"), None, None),
        check_vma=False,
    )
```
